32 devices in a mesh: grp: 2 (over x), seq: 16 (over z, y, core).
Axes of the slice: x: 2, y: 2, z: 4, core: 2. Of those that a mesh axis runs over, the one named last changes fastest.
Arguments:
- queries: bfloat16 [256, 4096], P(('grp', 'seq')), parts along dimension 0, may hold values from -9 to 9
- question_keys: bfloat16 [256, 2048], P(('grp', 'seq')), parts along dimension 0, may hold values from -4 to 4
- question_values: bfloat16 [256, 2048], P(('grp', 'seq')), parts along dimension 0, may hold values from -5 to 5
- doc_keys: bfloat16 [16384, 2048], P(('grp', 'seq')), parts along dimension 0, may hold values from -4 to 4
- doc_values: bfloat16 [16384, 2048], P(('grp', 'seq')), parts along dimension 0, may hold values from -5 to 5
- lengths: int32 [2], P('grp'), parts along dimension 0, may hold values from 4 to 128
- offsets: int32 [2], P('grp'), parts along dimension 0, may hold values from 2 to 8192, as said below
Outputs:
- attended: bfloat16 [256, 4096], P(('grp', 'seq')), parts along dimension 0
The draws below stay inside these ranges and needn't reach their ends.
There are 2 independent parts, one for each index of `grp`. The reference program is written for one: setup_inputs(seed, part) draws one part's arguments, and reference() takes and returns one part's arrays. A program takes and returns all parts, laid end to end along the dimension named above; each array names one. Nothing has to cross between parts.
Inputs may be any that keep to these rules, and one draw needn't show every extreme that they name: Some question has offsets equal to 8192.
All inputs are finite; a program needn't handle non-finite values.
Results may differ from the reference program's by a relative error of at most 0.0029.
Values may be sent and summed in bfloat16 or wider, within the bound.
A program may use at most 64 MiB of HBM per device.

```python
import jax
import jax.numpy as jnp
from jax import lax

H = 32
KVH = 16
HD = 128
QSCALE = 144
QL = 128
NQ = 1
DOC_DEV = 512
QT = 128
DOC = 8192
N_SEQ = 16


def draw_queries(key, part):
    values = 3.0 * jax.random.normal(jax.random.fold_in(key, 11), (NQ * QL, H * HD), jnp.float32)
    values = jnp.clip(values, -9.0, 9.0)
    return values.astype(jnp.bfloat16)


def draw_doc_keys(key, part):
    values = jax.random.normal(jax.random.fold_in(key, 13), (DOC, KVH * HD), jnp.float32)
    values = jnp.clip(values, -4.0, 4.0)
    return values.astype(jnp.bfloat16)


def draw_offsets(key, part):
    spread = jax.random.randint(jax.random.fold_in(key, 3), (NQ,), 0, DOC - 1)
    shifts = jax.random.randint(jax.random.fold_in(key, 5), (NQ,), 0, 11)
    result = 2 + jnp.right_shift(spread, shifts)
    chosen = jax.random.randint(jax.random.fold_in(key, 9), (), 0, NQ)
    result = jnp.where(jnp.arange(NQ, dtype=jnp.int32) == chosen, DOC, result)
    return result.astype(jnp.int32)


def levels(rng, dims, split, least, top_value):
    def one(dim, parts):
        heights = jax.random.uniform(jax.random.fold_in(jax.random.fold_in(rng, 6), dim), (parts,), jnp.float32, least / len(split), top_value / len(split))
        return jnp.repeat(jnp.exp(heights), dims[dim] // parts).reshape((-1,) + (1,) * (len(dims) - dim - 1))

    loudness = one(*split[0])
    for cut in split[1:]:
        loudness = loudness * one(*cut)
    return loudness


def normal_values(key, dims, width, most, shards=(), held_as=jnp.bfloat16):
    values = width * jax.random.normal(key, dims, jnp.float32)
    if shards:
        values = values * levels(key, dims, shards, -0.22, 0.18)
    return jnp.clip(values, -most, most).astype(held_as)


def setup_inputs(seed: int = 0, part: int = 0) -> dict:
    keys = jax.random.split(jax.random.key(seed), 8)
    part_keys = jax.random.split(jax.random.fold_in(keys[7], part), 8)
    queries = draw_queries(jax.random.fold_in(jax.random.fold_in(keys[7], part), 71), part)
    question_keys = normal_values(part_keys[1], (QT, KVH * HD), 1.0, 4.0, ((0, 16),))
    question_values = normal_values(part_keys[2], (QT, KVH * HD), 1.0, 5.0, ((0, 16),))
    doc_keys = draw_doc_keys(jax.random.fold_in(jax.random.fold_in(keys[7], part), 71), part)
    doc_values = normal_values(part_keys[4], (DOC, KVH * HD), 1.0, 5.0, ((0, 16),))
    lengths = jax.random.randint(part_keys[5], (NQ,), 4, QL + 1).astype(jnp.int32)
    offsets = draw_offsets(jax.random.fold_in(jax.random.fold_in(keys[7], part), 71), part)
    return {"queries": queries, "question_keys": question_keys, "question_values": question_values, "doc_keys": doc_keys, "doc_values": doc_values, "lengths": lengths, "offsets": offsets}


MASKED = -1.0e30


def row_tables(start, count, lengths, offsets):
    rows = start + jnp.arange(count, dtype=jnp.int32)
    question = rows // QL
    position = rows % QL
    owner_table = question[:, None] == jnp.arange(NQ, dtype=jnp.int32)[None, :]
    row_length = jnp.sum(jnp.where(owner_table, lengths[None, :], 0), axis=1)
    row_offset = jnp.sum(jnp.where(owner_table, offsets[None, :], 0), axis=1)
    return question, position, position < row_length, row_offset


def rounded(values):
    narrow = lax.optimization_barrier(values.astype(jnp.bfloat16))
    return narrow.astype(jnp.float32)


def reference(queries, question_keys, question_values, doc_keys, doc_values, lengths, offsets):
    total_rows = NQ * QL
    rows_block = total_rows // N_SEQ
    per_group = H // KVH
    factor_q = QSCALE ** -0.5
    question, position, live_rows, row_offset = row_tables(0, total_rows, lengths, offsets)
    query_all = queries.astype(jnp.float32).reshape(total_rows, KVH, per_group, HD)

    def visit(state, block):
        row_top, numer, denom = state
        doc_start = (block * DOC_DEV).astype(jnp.int32)
        self_start = (block * rows_block).astype(jnp.int32)
        key_doc = lax.dynamic_slice_in_dim(doc_keys, doc_start, DOC_DEV, 0).astype(jnp.float32).reshape(DOC_DEV, KVH, HD)
        value_doc = lax.dynamic_slice_in_dim(doc_values, doc_start, DOC_DEV, 0).astype(jnp.float32).reshape(DOC_DEV, KVH, HD)
        key_self = lax.dynamic_slice_in_dim(question_keys, self_start, rows_block, 0).astype(jnp.float32).reshape(rows_block, KVH, HD)
        value_self = lax.dynamic_slice_in_dim(question_values, self_start, rows_block, 0).astype(jnp.float32).reshape(rows_block, KVH, HD)
        doc_places = doc_start + jnp.arange(DOC_DEV, dtype=jnp.int32)
        self_rows = self_start + jnp.arange(rows_block, dtype=jnp.int32)
        mask_doc = live_rows[:, None] & (doc_places[None, :] < row_offset[:, None])
        mask_self = live_rows[:, None] & (self_rows[None, :] // QL == question[:, None]) & (self_rows[None, :] % QL <= position[:, None])
        mask_doc = mask_doc[:, None, None, :]
        mask_self = mask_self[:, None, None, :]
        scores_doc = jnp.einsum("rgjd,kgd->rgjk", query_all, key_doc) * factor_q
        scores_self = jnp.einsum("rgjd,kgd->rgjk", query_all, key_self) * factor_q
        scores_doc = jnp.where(mask_doc, scores_doc, MASKED)
        scores_self = jnp.where(mask_self, scores_self, MASKED)
        block_top = jnp.maximum(jnp.max(scores_doc, axis=-1), jnp.max(scores_self, axis=-1))
        weights_doc = rounded(jnp.where(mask_doc, jnp.exp(scores_doc - block_top[..., None]), 0.0))
        weights_self = rounded(jnp.where(mask_self, jnp.exp(scores_self - block_top[..., None]), 0.0))
        block_num = jnp.einsum("rgjk,kgd->rgjd", weights_doc, value_doc) + jnp.einsum("rgjk,kgd->rgjd", weights_self, value_self)
        block_den = jnp.sum(weights_doc, axis=-1) + jnp.sum(weights_self, axis=-1)
        new_top = jnp.maximum(row_top, block_top)
        old_factor = jnp.exp(row_top - new_top)
        new_factor = jnp.exp(block_top - new_top)
        numer = numer * old_factor[..., None] + block_num * new_factor[..., None]
        denom = denom * old_factor + block_den * new_factor
        return (new_top, numer, denom), None

    start_state = (jnp.full((total_rows, KVH, per_group), MASKED, jnp.float32),
                   jnp.zeros((total_rows, KVH, per_group, HD), jnp.float32),
                   jnp.zeros((total_rows, KVH, per_group), jnp.float32))
    final_state, unused = lax.scan(visit, start_state, jnp.arange(N_SEQ, dtype=jnp.int32))
    row_top, numer, denom = final_state
    safe_den = jnp.where(live_rows[:, None, None], denom, 1.0)
    result = numer / safe_den[..., None]
    result = jnp.where(live_rows[:, None, None, None], result, 0.0)
    return result.reshape(total_rows, H * HD).astype(jnp.bfloat16)
```

```python
import functools
import math

import jax
import jax.numpy as jnp
from jax import lax
from jax.experimental import pallas as pl
from jax.experimental.pallas import tpu as pltpu
from jax.sharding import PartitionSpec as P

H = 32
KVH = 16
HD = 128
QSCALE = 144
QL = 128
NQ = 1


MASKED = -1e30


def row_tables(start, count, lengths, offsets):
    rows = start + jnp.arange(count, dtype=jnp.int32)
    question = rows // QL
    position = rows % QL
    owner_table = question[:, None] == jnp.arange(NQ, dtype=jnp.int32)[None, :]
    row_length = jnp.sum(jnp.where(owner_table, lengths[None, :], 0), axis=1)
    row_offset = jnp.sum(jnp.where(owner_table, offsets[None, :], 0), axis=1)
    return (question, position, position < row_length, row_offset)


def local(queries, question_keys, question_values, doc_keys, doc_values, lengths, offsets):
    rows_local = queries.shape[0]
    doc_local = doc_keys.shape[0]
    device_count = lax.axis_size("seq")
    device_index = lax.axis_index("seq")
    total_rows = rows_local * device_count
    per_group = H // KVH
    factor_q = QSCALE ** (-0.5)
    key_doc = doc_keys.reshape(doc_local, KVH, HD)
    value_doc = doc_values.reshape(doc_local, KVH, HD)
    key_self = question_keys.reshape(rows_local, KVH, HD)
    value_self = question_values.reshape(rows_local, KVH, HD)
    doc_places = device_index * doc_local + jnp.arange(doc_local, dtype=jnp.int32)
    self_rows = device_index * rows_local + jnp.arange(rows_local, dtype=jnp.int32)
    whole = lax.all_gather(queries, "seq", axis=0, tiled=True)
    block_rows = math.gcd(total_rows, 512)
    block_count = total_rows // block_rows

    def one_block(start):
        piece = whole.reshape(block_rows, KVH, per_group, HD)
        question, position, live_rows, row_offset = row_tables(start, block_rows, lengths, offsets)
        mask_doc = live_rows[:, None] & (doc_places[None, :] < row_offset[:, None])
        mask_self = (
            live_rows[:, None]
            & (self_rows[None, :] // QL == question[:, None])
            & (self_rows[None, :] % QL <= position[:, None])
        )
        mask_doc = mask_doc[:, None, None, :]
        mask_self = mask_self[:, None, None, :]
        scores_doc = (
            jnp.einsum("rgjd,kgd->rgjk", piece, key_doc, preferred_element_type=jnp.float32)
            * factor_q
        )
        scores_self = (
            jnp.einsum("rgjd,kgd->rgjk", piece, key_self, preferred_element_type=jnp.float32)
            * factor_q
        )
        scores_doc = jnp.where(mask_doc, scores_doc, MASKED)
        scores_self = jnp.where(mask_self, scores_self, MASKED)
        block_top = jnp.maximum(jnp.max(scores_doc, axis=-1), jnp.max(scores_self, axis=-1))
        weights_doc = jnp.where(mask_doc, jnp.exp(scores_doc - block_top[..., None]), 0.0).astype(
            jnp.bfloat16
        )
        weights_self = jnp.where(
            mask_self, jnp.exp(scores_self - block_top[..., None]), 0.0
        ).astype(jnp.bfloat16)
        block_den = jnp.sum(weights_doc.astype(jnp.float32), axis=-1) + jnp.sum(
            weights_self.astype(jnp.float32), axis=-1
        )
        block_num = jnp.einsum(
            "rgjk,kgd->rgjd", weights_doc, value_doc, preferred_element_type=jnp.float32
        )
        block_num = block_num + jnp.einsum(
            "rgjk,kgd->rgjd", weights_self, value_self, preferred_element_type=jnp.float32
        )
        return (
            block_num.reshape(block_rows, H * HD),
            block_top.reshape(block_rows, H),
            block_den.reshape(block_rows, H),
        )

    starts = jnp.arange(block_count, dtype=jnp.int32) * block_rows
    numer, row_top, denom = lax.map(one_block, starts)
    numer = numer.reshape(total_rows, H * HD)
    row_top = row_top.reshape(total_rows, H)
    denom = denom.reshape(total_rows, H)
    got_num, got_top, got_den = (
        lax.all_to_all(numer[None], "seq", split_axis=1, concat_axis=0, tiled=True),
        lax.all_to_all(row_top[None], "seq", split_axis=1, concat_axis=0, tiled=True),
        lax.all_to_all(denom[None], "seq", split_axis=1, concat_axis=0, tiled=True),
    )
    overall = jnp.max(got_top, axis=0)
    rescale = jnp.exp(got_top - overall[None])
    total_num = jnp.sum(
        got_num.reshape(device_count, rows_local, H, HD) * rescale[:, :, :, None], axis=0
    )
    total_den = jnp.sum(got_den * rescale, axis=0)
    question, position, live_rows, row_offset = row_tables(
        device_index * rows_local, rows_local, lengths, offsets
    )
    safe_den = jnp.where(live_rows[:, None], total_den, 1.0)
    result = (total_num / safe_den[:, :, None]).reshape(rows_local, H * HD)
    return jnp.where(live_rows[:, None], result, 0.0).astype(jnp.bfloat16)


MESH = pl.DeviceIdType.MESH
LANE = 128
CHUNKS = 4
LOG2E = math.log2(math.e)
WIRE = jnp.int16
WIRE_TOP = 32767.0
HALF_KVH = KVH // 2
PER_GROUP = H // KVH
GROUPS = HALF_KVH // CHUNKS
STATS = 8


def fused_kernel(
    n, q_hbm, qk_hbm, qv_hbm, k_hbm, v_hbm, len_hbm, off_hbm, o_ref,
    qown, qbuf, kself, vself, kbuf, vt, bias_doc, bias_self, scores, len_ref, off_ref, vbuf,
    nkeep, skeep, nsend, ssend, narr, sarr, wsend, wstat, warr, wsarr,
    q_sem, in_sem, kv_sem, kv_send, kv_recv,
    zq_send, zq_recv, yq_send, yq_recv, pq_send, pq_recv, f_send, f_recv,
    p_send, p_recv, w_send, w_recv,
):
    length = n // 4
    rows = q_hbm.shape[0]
    doc = k_hbm.shape[0]
    docs = 2 * doc
    selves = 2 * rows
    half_kv = HALF_KVH * HD
    half_q = half_kv * PER_GROUP
    kv_wide = GROUPS * HD
    wide = kv_wide * PER_GROUP
    side = length * 2 * rows
    me = lax.axis_index("seq")
    core = lax.rem(me, 2)
    chip = me // 2
    y = lax.rem(chip, 2)
    z = chip // 2

    def device(zz, yy, cc):
        return {"seq": (zz * 2 + yy) * 2 + cc}

    def zpeer(d):
        return lax.rem(z + d, length)

    barrier = pltpu.get_barrier_semaphore()
    peers = [device(z, y, 1 - core)] + [device(z, 1 - y, cc) for cc in range(2)]
    peers += [device(zpeer(d), y, cc) for d in range(1, length) for cc in range(2)]
    for peer in peers:
        pl.semaphore_signal(barrier, inc=1, device_id=peer, device_id_type=MESH)

    q_in = pltpu.make_async_copy(q_hbm, qown, q_sem.at[CHUNKS])
    q_in.start()
    small = [
        pltpu.make_async_copy(len_hbm, len_ref, in_sem.at[0]),
        pltpu.make_async_copy(off_hbm, off_ref, in_sem.at[1]),
        pltpu.make_async_copy(qk_hbm.at[:, pl.ds(core * half_kv, half_kv)], kself.at[core], in_sem.at[2]),
        pltpu.make_async_copy(qv_hbm.at[:, pl.ds(core * half_kv, half_kv)], vself.at[core], in_sem.at[3]),
    ]
    for copy in small:
        copy.start()

    def q_own(c):
        return pltpu.make_async_copy(
            q_hbm.at[:, pl.ds(core * half_q + c * wide, wide)], qbuf.at[c, y, z, core], q_sem.at[c]
        )

    def kv_local(c):
        cols = pl.ds(core * half_kv + c * kv_wide, kv_wide)
        at = pl.ds(core * doc, doc)
        to = pl.ds(c * kv_wide, kv_wide)
        return (
            pltpu.make_async_copy(k_hbm.at[:, cols], kbuf.at[at, to], kv_sem.at[0, c]),
            pltpu.make_async_copy(v_hbm.at[:, cols], vbuf.at[at, to], kv_sem.at[1, c]),
        )

    def kv_remote(c):
        cols = pl.ds((1 - core) * half_kv + c * kv_wide, kv_wide)
        at = pl.ds(core * doc, doc)
        to = pl.ds(c * kv_wide, kv_wide)
        return tuple(
            pltpu.make_async_remote_copy(
                a.at[:, cols], b.at[at, to], kv_send.at[i, c], kv_recv.at[i, c],
                device_id=device(z, y, 1 - core), device_id_type=MESH,
            )
            for i, (a, b) in enumerate(((k_hbm, kbuf), (v_hbm, vbuf)))
        )

    def self_remote():
        cols = pl.ds((1 - core) * half_kv, half_kv)
        return tuple(
            pltpu.make_async_remote_copy(
                a.at[:, cols], b.at[core], kv_send.at[i, CHUNKS], kv_recv.at[i, CHUNKS],
                device_id=device(z, y, 1 - core), device_id_type=MESH,
            )
            for i, (a, b) in enumerate(((qk_hbm, kself), (qv_hbm, vself)))
        )

    def q_piece(c, cc):
        return qown.at[:, pl.ds(cc * half_q + c * wide, wide)]

    def zq(c, d, cc):
        return pltpu.make_async_remote_copy(
            q_piece(c, cc), qbuf.at[c, y, z, core], zq_send.at[c, d, cc], zq_recv.at[c, d, core],
            device_id=device(zpeer(d), y, cc), device_id_type=MESH,
        )

    def zq_wait(c, d):
        for cc in range(2):
            pltpu.make_async_remote_copy(
                q_piece(c, cc), qbuf.at[c, y, zpeer(length - d), cc],
                zq_send.at[c, d, cc], zq_recv.at[c, d, cc],
                device_id=device(zpeer(d), y, cc), device_id_type=MESH,
            ).wait_recv()

    def yq(c, cc):
        return pltpu.make_async_remote_copy(
            q_piece(c, cc), qbuf.at[c, y, z, core], yq_send.at[c, cc], yq_recv.at[c, core],
            device_id=device(z, 1 - y, cc), device_id_type=MESH,
        )

    def yq_wait(c):
        for cc in range(2):
            pltpu.make_async_remote_copy(
                q_piece(c, cc), qbuf.at[c, 1 - y, z, cc], yq_send.at[c, cc], yq_recv.at[c, cc],
                device_id=device(z, 1 - y, cc), device_id_type=MESH,
            ).wait_recv()

    def pq(c):
        return pltpu.make_async_remote_copy(
            q_piece(c, 1 - core), qbuf.at[c, y, z, core], pq_send.at[c], pq_recv.at[c],
            device_id=device(z, y, 1 - core), device_id_type=MESH,
        )

    def forward(c, d):
        at = zpeer(length - d)
        return pltpu.make_async_remote_copy(
            qbuf.at[c, y, at], qbuf.at[c, y, at], f_send.at[c, d], f_recv.at[c, d],
            device_id=device(z, 1 - y, core), device_id_type=MESH,
        )

    def p_copies(c):
        return tuple(
            pltpu.make_async_remote_copy(
                a.at[c], b.at[c], p_send.at[c, i], p_recv.at[c, i],
                device_id=device(z, 1 - y, core), device_id_type=MESH,
            )
            for i, (a, b) in enumerate(((nsend, narr), (ssend, sarr)))
        )

    def w_copy(c, d, cc):
        return pltpu.make_async_remote_copy(
            wsend.at[c, zpeer(d), cc], warr.at[c, z, core], w_send.at[c, d, cc], w_recv.at[c, d, core],
            device_id=device(zpeer(d), y, cc), device_id_type=MESH,
        )

    def s_copy(d, cc):
        return pltpu.make_async_remote_copy(
            wstat.at[zpeer(d), cc], wsarr.at[z, core],
            w_send.at[CHUNKS, d, cc], w_recv.at[CHUNKS, d, core],
            device_id=device(zpeer(d), y, cc), device_id_type=MESH,
        )

    def wp_copy(c):
        return pltpu.make_async_remote_copy(
            wsend.at[c, z, 1 - core], warr.at[c, z, core], w_send.at[c, 0, 0], w_recv.at[c, 0, 0],
            device_id=device(z, y, 1 - core), device_id_type=MESH,
        )

    def sp_copy():
        return pltpu.make_async_remote_copy(
            wstat.at[z, 1 - core], wsarr.at[z, core],
            w_send.at[CHUNKS, 0, 0], w_recv.at[CHUNKS, 0, 0],
            device_id=device(z, y, 1 - core), device_id_type=MESH,
        )

    for c in range(CHUNKS):
        q_own(c).start()
        for copy in kv_local(c):
            copy.start()
    q_in.wait()
    pl.semaphore_wait(barrier, len(peers))

    for c in range(CHUNKS):
        for d in range(1, length):
            for cc in range(2):
                zq(c, d, cc).start()
        for cc in range(2):
            yq(c, cc).start()
        pq(c).start()
    for copy in self_remote():
        copy.start()
    for c in range(CHUNKS):
        for copy in reversed(kv_remote(c)):
            copy.start()

    for copy in small:
        copy.wait()
    place = chip * docs + lax.broadcasted_iota(jnp.int32, (docs, LANE), 0)
    bias_doc[...] = jnp.where(place < off_ref[0], 0.0, MASKED)
    spot = lax.broadcasted_iota(jnp.int32, (selves, 2 * LANE), 1)
    key_row = chip * selves + lax.broadcasted_iota(jnp.int32, (selves, 2 * LANE), 0)
    inner = spot % side
    row = ((inner // (2 * rows)) * 2 + jnp.where(spot < LANE, y, 1 - y)) * (2 * rows) + inner % (2 * rows)
    bias_self[...] = jnp.where(key_row <= row, 0.0, MASKED)
    for copy in self_remote():
        copy.wait_recv()
    kbuf[docs:, :] = kself[...].astype(jnp.float32).reshape(selves, half_kv).astype(kbuf.dtype)
    vbuf[docs:, :] = vself[...].astype(jnp.float32).reshape(selves, half_kv).astype(kbuf.dtype)
    ones = lax.broadcasted_iota(jnp.int32, (16, docs + LANE), 0) == 0
    ones = jnp.where(ones, 1.0, 0.0).astype(vt.dtype)
    for g in range(HALF_KVH):
        vt[g, HD:, :] = ones

    def turn(c):
        for copy in kv_local(c):
            copy.wait()
        for copy in kv_remote(c):
            copy.wait_recv()
        for g in range(GROUPS):
            cols = slice((c * GROUPS + g) * HD, (c * GROUPS + g + 1) * HD)
            vt[c * GROUPS + g, :HD, :docs] = vbuf[:docs, cols].T
            last = vbuf[docs:, cols].astype(jnp.float32)
            last = jnp.concatenate([last, jnp.zeros((LANE - selves, HD), jnp.float32)], axis=0)
            vt[c * GROUPS + g, :HD, docs:] = last.T.astype(vt.dtype)

    def relay(c):
        for d in range(1, length):
            zq_wait(c, d)
            forward(c, d).start()

    factor = QSCALE ** (-0.5) * LOG2E
    tile = 256

    def attend(c):
        q_own(c).wait()
        pq(c).wait_recv()
        yq_wait(c)
        for d in range(1, length):
            forward(c, d).wait_recv()
        for g in range(GROUPS):
            at = c * GROUPS + g
            cols = slice(at * HD, (at + 1) * HD)
            pieces = []
            for yy in (y, 1 - y):
                for j in range(PER_GROUP):
                    h = g * PER_GROUP + j
                    block = qbuf[c, yy, :, :, :, h * HD : (h + 1) * HD].astype(jnp.float32)
                    pieces.append(block.reshape(side, HD).astype(jnp.bfloat16))
            query = jnp.concatenate(pieces, axis=0)
            top = None
            for start in list(range(0, docs, tile)) + [docs]:
                size = tile if start < docs else selves
                part = lax.dot_general(
                    kbuf[start : start + size, cols], query, (((1,), (1,)), ((), ())),
                    preferred_element_type=jnp.float32,
                )
                if start < docs:
                    mask = bias_doc[start : start + size, :]
                    part = part + jnp.concatenate([mask, mask], axis=1)
                else:
                    part = part + bias_self[...]
                scores[at % 2, start : start + size, :] = part
                most = jnp.max(part.reshape(size // 8, 8, 2 * LANE), axis=0)
                top = most if top is None else jnp.maximum(top, most)
            top = jnp.max(top, axis=0, keepdims=True)
            total = None
            for start in list(range(0, docs, tile)) + [docs]:
                size = tile if start < docs else selves
                part = scores[at % 2, start : start + size, :]
                weights = jnp.exp2((part - top) * factor)
                span = size
                if start == docs:
                    span = LANE
                    weights = jnp.concatenate(
                        [weights, jnp.zeros((LANE - selves, 2 * LANE), jnp.float32)], axis=0
                    )
                got = jnp.dot(
                    vt[at, :, start : start + span], weights.astype(jnp.bfloat16),
                    preferred_element_type=jnp.float32,
                )
                total = got if total is None else total + got
            top = top * factor
            den = total[HD : HD + 1]
            num = total[:HD]
            nkeep[c, g * HD : (g + 1) * HD, :] = num[:, :LANE]
            skeep[c, 3 * g : 3 * g + 1, :] = top[:, :LANE]
            skeep[c, 3 * g + 1 : 3 * g + 2, :] = den[:, :LANE]
            out = num[:, LANE:]
            largest = jnp.maximum(jnp.max(jnp.abs(out), axis=0, keepdims=True), 1e-30)
            nsend[c, g * HD : (g + 1) * HD, :] = encode(out * (WIRE_TOP / largest))
            ssend[c, 3 * g : 3 * g + 1, :] = top[:, LANE:]
            ssend[c, 3 * g + 1 : 3 * g + 2, :] = den[:, LANE:]
            ssend[c, 3 * g + 2 : 3 * g + 3, :] = largest * (1.0 / WIRE_TOP)
        for copy in p_copies(c):
            copy.start()

    def pair_up(c):
        for copy in p_copies(c):
            copy.wait_recv()
        stats = []
        for g in range(GROUPS):
            top_a, top_b = skeep[c, 3 * g : 3 * g + 1, :], sarr[c, 3 * g : 3 * g + 1, :]
            top = jnp.maximum(top_a, top_b)
            fa, fb = jnp.exp2(top_a - top), jnp.exp2(top_b - top)
            den = skeep[c, 3 * g + 1 : 3 * g + 2, :] * fa + sarr[c, 3 * g + 1 : 3 * g + 2, :] * fb
            fb = fb * sarr[c, 3 * g + 2 : 3 * g + 3, :]
            span = slice(g * HD, (g + 1) * HD)
            num = nkeep[c, span, :] * fa + decode(narr[c, span, :]) * fb
            largest = jnp.maximum(jnp.max(jnp.abs(num), axis=0, keepdims=True), 1e-30)
            codes = encode((num * (WIRE_TOP / largest)).T)
            for j in range(PER_GROUP):
                h = g * PER_GROUP + j
                wsend[c, :, :, :, h * HD : (h + 1) * HD] = codes[j * side : (j + 1) * side].reshape(
                    length, 2, rows, HD
                )
            stats += [top, den, largest * (1.0 / WIRE_TOP)]
        stats.append(jnp.zeros((LANE - 3 * GROUPS, LANE), jnp.float32))
        table = jnp.concatenate(stats, axis=0).T
        for j in range(PER_GROUP):
            at = (c * PER_GROUP + j) * STATS
            wstat[:, :, :, at : at + STATS] = table[j * side : (j + 1) * side, :STATS].reshape(
                length, 2, rows, STATS
            )
        for d in range(1, length):
            for cc in range(2):
                if c == CHUNKS - 1:
                    s_copy(d, cc).start()
                w_copy(c, d, cc).start()
        wp_copy(c).start()
        warr[c, z, core] = wsend[c, z, core]
        if c == CHUNKS - 1:
            sp_copy().start()
            wsarr[z, core] = wstat[z, core]

    relay(0)
    turn(0)
    for c in range(CHUNKS):
        if c + 1 < CHUNKS:
            relay(c + 1)
        attend(c)
        if c + 1 < CHUNKS:
            turn(c + 1)
        if c > 0:
            pair_up(c - 1)
    pair_up(CHUNKS - 1)

    mine = me * rows + lax.broadcasted_iota(jnp.int32, (rows, HD), 0)
    live = mine % QL < len_ref[0]

    def w_wait(c, d):
        for cc in range(2):
            pltpu.make_async_remote_copy(
                wsend.at[c, zpeer(d), cc] if c < CHUNKS else wstat.at[zpeer(d), cc],
                warr.at[c, zpeer(length - d), cc] if c < CHUNKS else wsarr.at[zpeer(length - d), cc],
                w_send.at[c, d, cc], w_recv.at[c, d, cc],
                device_id=device(zpeer(d), y, cc), device_id_type=MESH,
            ).wait_recv()

    sp_copy().wait_recv()
    for d in range(1, length):
        w_wait(CHUNKS, d)
    for c in range(CHUNKS):
        wp_copy(c).wait_recv()
        for d in range(1, length):
            w_wait(c, d)
        for cc in range(2):
            for h in range(GROUPS * PER_GROUP):
                g, j = h // PER_GROUP, h % PER_GROUP
                at = (c * PER_GROUP + j) * STATS + 3 * g
                tops = [wsarr[k, cc, :, at : at + 1] for k in range(length)]
                overall = functools.reduce(jnp.maximum, tops)
                shrink = [jnp.exp2(t - overall) for t in tops]
                den = sum(wsarr[k, cc, :, at + 1 : at + 2] * shrink[k] for k in range(length))
                acc = jnp.zeros((rows, HD), jnp.float32)
                for k in range(length):
                    coef = wsarr[k, cc, :, at + 2 : at + 3] * shrink[k] / den
                    acc = acc + decode(warr[c, k, cc, :, h * HD : (h + 1) * HD]) * coef
                to = cc * half_q + c * wide + h * HD
                o_ref[:, to : to + HD] = jnp.where(live, acc, 0.0).astype(o_ref.dtype)

    for copy in self_remote():
        copy.wait_send()
    sp_copy().wait_send()
    for c in range(CHUNKS):
        for copy in kv_remote(c) + p_copies(c):
            copy.wait_send()
        pq(c).wait_send()
        wp_copy(c).wait_send()
        for cc in range(2):
            yq(c, cc).wait_send()
        for d in range(1, length):
            forward(c, d).wait_send()
            for cc in range(2):
                zq(c, d, cc).wait_send()
                w_copy(c, d, cc).wait_send()
    for d in range(1, length):
        for cc in range(2):
            s_copy(d, cc).wait_send()


def encode(x):
    return jnp.round(x).astype(jnp.int32).astype(WIRE)


def decode(x):
    return x.astype(jnp.int32).astype(jnp.float32)


def fused(n, queries, question_keys, question_values, doc_keys, doc_values, lengths, offsets):
    rows = queries.shape[0]
    doc = doc_keys.shape[0]
    if (
        NQ != 1 or n % 4 or n < 8 or rows % 8 or n * rows * PER_GROUP != 2 * LANE
        or doc % LANE or doc > 1024 or n * rows != QL
    ):
        return local(
            queries, question_keys, question_values, doc_keys, doc_values, lengths, offsets
        )
    length = n // 4
    docs, selves = 2 * doc, 2 * rows
    half_kv = HALF_KVH * HD
    wide = GROUPS * PER_GROUP * HD
    vmem = pl.BlockSpec(memory_space=pltpu.VMEM)
    hbm = pl.BlockSpec(memory_space=pl.ANY)
    f32, bf16 = jnp.float32, jnp.bfloat16
    dma = pltpu.SemaphoreType.DMA
    return pl.pallas_call(
        functools.partial(fused_kernel, n),
        out_shape=jax.ShapeDtypeStruct(queries.shape, bf16),
        in_specs=[hbm] * 7,
        out_specs=vmem,
        scratch_shapes=[
            pltpu.VMEM((rows, H * HD), bf16),
            pltpu.VMEM((CHUNKS, 2, length, 2, rows, wide), bf16),
            pltpu.VMEM((2, rows, half_kv), bf16),
            pltpu.VMEM((2, rows, half_kv), bf16),
            pltpu.VMEM((docs + selves, half_kv), bf16),
            pltpu.VMEM((HALF_KVH, HD + 16, docs + LANE), bf16),
            pltpu.VMEM((docs, LANE), f32),
            pltpu.VMEM((selves, 2 * LANE), f32),
            pltpu.VMEM((2, docs + selves, 2 * LANE), f32),
            pltpu.SMEM((1,), jnp.int32),
            pltpu.SMEM((1,), jnp.int32),
            pltpu.VMEM((docs + selves, half_kv), bf16),
            pltpu.VMEM((CHUNKS, GROUPS * HD, LANE), f32),
            pltpu.VMEM((CHUNKS, STATS, LANE), f32),
            pltpu.VMEM((CHUNKS, GROUPS * HD, LANE), WIRE),
            pltpu.VMEM((CHUNKS, STATS, LANE), f32),
            pltpu.VMEM((CHUNKS, GROUPS * HD, LANE), WIRE),
            pltpu.VMEM((CHUNKS, STATS, LANE), f32),
            pltpu.VMEM((CHUNKS, length, 2, rows, wide), WIRE),
            pltpu.VMEM((length, 2, rows, LANE), f32),
            pltpu.VMEM((CHUNKS, length, 2, rows, wide), WIRE),
            pltpu.VMEM((length, 2, rows, LANE), f32),
            dma((CHUNKS + 1,)),
            dma((4,)),
            dma((2, CHUNKS)),
            dma((2, CHUNKS + 1)),
            dma((2, CHUNKS + 1)),
            dma((CHUNKS, length, 2)),
            dma((CHUNKS, length, 2)),
            dma((CHUNKS, 2)),
            dma((CHUNKS, 2)),
            dma((CHUNKS,)),
            dma((CHUNKS,)),
            dma((CHUNKS, length)),
            dma((CHUNKS, length)),
            dma((CHUNKS, 2)),
            dma((CHUNKS, 2)),
            dma((CHUNKS + 1, length, 2)),
            dma((CHUNKS + 1, length, 2)),
        ],
        compiler_params=pltpu.CompilerParams(
            collective_id=0, has_side_effects=True, vmem_limit_bytes=60 * 1024 * 1024
        ),
    )(queries, question_keys, question_values, doc_keys, doc_values, lengths, offsets)


def solution(mesh):
    placed = (
        P(("grp", "seq"), None),
        P(("grp", "seq"), None),
        P(("grp", "seq"), None),
        P(("grp", "seq"), None),
        P(("grp", "seq"), None),
        P("grp"),
        P("grp"),
    )
    return jax.shard_map(
        functools.partial(fused, mesh.shape["seq"]),
        mesh=mesh, in_specs=placed, out_specs=P(("grp", "seq"), None), check_vma=False,
    )
```

```python
import functools
import math

import jax
import jax.numpy as jnp
from jax import lax
from jax.experimental import pallas as pl
from jax.experimental.pallas import tpu as pltpu
from jax.sharding import PartitionSpec as P

H = 32
KVH = 16
HD = 128
QSCALE = 144
QL = 128
NQ = 1


MASKED = -1e30


def row_tables(start, count, lengths, offsets):
    rows = start + jnp.arange(count, dtype=jnp.int32)
    question = rows // QL
    position = rows % QL
    owner_table = question[:, None] == jnp.arange(NQ, dtype=jnp.int32)[None, :]
    row_length = jnp.sum(jnp.where(owner_table, lengths[None, :], 0), axis=1)
    row_offset = jnp.sum(jnp.where(owner_table, offsets[None, :], 0), axis=1)
    return (question, position, position < row_length, row_offset)


def local(queries, question_keys, question_values, doc_keys, doc_values, lengths, offsets):
    rows_local = queries.shape[0]
    doc_local = doc_keys.shape[0]
    device_count = lax.axis_size("seq")
    device_index = lax.axis_index("seq")
    total_rows = rows_local * device_count
    per_group = H // KVH
    factor_q = QSCALE ** (-0.5)
    key_doc = doc_keys.reshape(doc_local, KVH, HD)
    value_doc = doc_values.reshape(doc_local, KVH, HD)
    key_self = question_keys.reshape(rows_local, KVH, HD)
    value_self = question_values.reshape(rows_local, KVH, HD)
    doc_places = device_index * doc_local + jnp.arange(doc_local, dtype=jnp.int32)
    self_rows = device_index * rows_local + jnp.arange(rows_local, dtype=jnp.int32)
    whole = lax.all_gather(queries, "seq", axis=0, tiled=True)
    block_rows = math.gcd(total_rows, 512)
    block_count = total_rows // block_rows

    def one_block(start):
        piece = whole.reshape(block_rows, KVH, per_group, HD)
        question, position, live_rows, row_offset = row_tables(start, block_rows, lengths, offsets)
        mask_doc = live_rows[:, None] & (doc_places[None, :] < row_offset[:, None])
        mask_self = (
            live_rows[:, None]
            & (self_rows[None, :] // QL == question[:, None])
            & (self_rows[None, :] % QL <= position[:, None])
        )
        mask_doc = mask_doc[:, None, None, :]
        mask_self = mask_self[:, None, None, :]
        scores_doc = (
            jnp.einsum("rgjd,kgd->rgjk", piece, key_doc, preferred_element_type=jnp.float32)
            * factor_q
        )
        scores_self = (
            jnp.einsum("rgjd,kgd->rgjk", piece, key_self, preferred_element_type=jnp.float32)
            * factor_q
        )
        scores_doc = jnp.where(mask_doc, scores_doc, MASKED)
        scores_self = jnp.where(mask_self, scores_self, MASKED)
        block_top = jnp.maximum(jnp.max(scores_doc, axis=-1), jnp.max(scores_self, axis=-1))
        weights_doc = jnp.where(mask_doc, jnp.exp(scores_doc - block_top[..., None]), 0.0).astype(
            jnp.bfloat16
        )
        weights_self = jnp.where(
            mask_self, jnp.exp(scores_self - block_top[..., None]), 0.0
        ).astype(jnp.bfloat16)
        block_den = jnp.sum(weights_doc.astype(jnp.float32), axis=-1) + jnp.sum(
            weights_self.astype(jnp.float32), axis=-1
        )
        block_num = jnp.einsum(
            "rgjk,kgd->rgjd", weights_doc, value_doc, preferred_element_type=jnp.float32
        )
        block_num = block_num + jnp.einsum(
            "rgjk,kgd->rgjd", weights_self, value_self, preferred_element_type=jnp.float32
        )
        return (
            block_num.reshape(block_rows, H * HD),
            block_top.reshape(block_rows, H),
            block_den.reshape(block_rows, H),
        )

    starts = jnp.arange(block_count, dtype=jnp.int32) * block_rows
    numer, row_top, denom = lax.map(one_block, starts)
    numer = numer.reshape(total_rows, H * HD)
    row_top = row_top.reshape(total_rows, H)
    denom = denom.reshape(total_rows, H)
    got_num, got_top, got_den = (
        lax.all_to_all(numer[None], "seq", split_axis=1, concat_axis=0, tiled=True),
        lax.all_to_all(row_top[None], "seq", split_axis=1, concat_axis=0, tiled=True),
        lax.all_to_all(denom[None], "seq", split_axis=1, concat_axis=0, tiled=True),
    )
    overall = jnp.max(got_top, axis=0)
    rescale = jnp.exp(got_top - overall[None])
    total_num = jnp.sum(
        got_num.reshape(device_count, rows_local, H, HD) * rescale[:, :, :, None], axis=0
    )
    total_den = jnp.sum(got_den * rescale, axis=0)
    question, position, live_rows, row_offset = row_tables(
        device_index * rows_local, rows_local, lengths, offsets
    )
    safe_den = jnp.where(live_rows[:, None], total_den, 1.0)
    result = (total_num / safe_den[:, :, None]).reshape(rows_local, H * HD)
    return jnp.where(live_rows[:, None], result, 0.0).astype(jnp.bfloat16)


MESH = pl.DeviceIdType.MESH
LANE = 128
CHUNKS = 4
PIECES = 2
LOG2E = math.log2(math.e)
WIRE = jnp.int16
WIRE_TOP = 32767.0
HALF_KVH = KVH // 2
PER_GROUP = H // KVH
GROUPS = HALF_KVH // CHUNKS
STATS = 8


def fused_kernel(
    n, q_hbm, qk_hbm, qv_hbm, k_hbm, v_hbm, len_ref, off_ref, o_ref,
    qown, qbuf, kself, vself, kbuf, vt, bias_doc, bias_self, scores, vbuf,
    nkeep, skeep, nsend, narr, wsend, warr, osend,
    q_sem, in_sem, kv_sem, kv_send, kv_recv,
    zq_send, zq_recv, yq_send, yq_recv, pq_send, pq_recv, f_send, f_recv,
    p_send, p_recv, w_send, w_recv, o_send, o_recv,
):
    length = n // 4
    rows = q_hbm.shape[0]
    doc = k_hbm.shape[0]
    docs = 2 * doc
    selves = 2 * rows
    half_kv = HALF_KVH * HD
    half_q = half_kv * PER_GROUP
    kv_wide = GROUPS * HD
    wide = kv_wide * PER_GROUP
    q_wide = half_q // PIECES
    side = length * 2 * rows
    me = lax.axis_index("seq")
    core = lax.rem(me, 2)
    chip = me // 2
    y = lax.rem(chip, 2)
    z = chip // 2
    others = (z + 1 - 2 * lax.rem(z, 2), 2 - z // 2, 3 - 3 * (z // 2))

    def device(zz, yy, cc):
        return {"seq": (zz * 2 + yy) * 2 + cc}

    barrier = pltpu.get_barrier_semaphore()
    peers = [device(zz, y, cc) for zz in others for cc in range(2)]
    peers += [device(z, 1 - y, cc) for cc in range(2)] + [device(z, y, 1 - core)]
    for peer in peers:
        pl.semaphore_signal(barrier, inc=1, device_id=peer, device_id_type=MESH)

    q_in = pltpu.make_async_copy(q_hbm, qown, q_sem.at[PIECES])
    q_in.start()
    small = [
        pltpu.make_async_copy(qk_hbm.at[:, pl.ds(core * half_kv, half_kv)], kself.at[core], in_sem.at[0]),
        pltpu.make_async_copy(qv_hbm.at[:, pl.ds(core * half_kv, half_kv)], vself.at[core], in_sem.at[1]),
    ]
    for copy in small:
        copy.start()

    def q_own(c):
        return pltpu.make_async_copy(
            q_hbm.at[:, pl.ds(core * half_q + c * q_wide, q_wide)], qbuf.at[c, y, z, core], q_sem.at[c]
        )

    def kv_local(c):
        cols = pl.ds(core * half_kv + c * kv_wide, kv_wide)
        at = pl.ds(core * doc, doc)
        to = pl.ds(c * kv_wide, kv_wide)
        return (
            pltpu.make_async_copy(k_hbm.at[:, cols], kbuf.at[at, to], kv_sem.at[0, c]),
            pltpu.make_async_copy(v_hbm.at[:, cols], vbuf.at[at, to], kv_sem.at[1, c]),
        )

    def kv_remote(c):
        cols = pl.ds((1 - core) * half_kv + c * kv_wide, kv_wide)
        at = pl.ds(core * doc, doc)
        to = pl.ds(c * kv_wide, kv_wide)
        return tuple(
            pltpu.make_async_remote_copy(
                a.at[:, cols], b.at[at, to], kv_send.at[i, c], kv_recv.at[i, c],
                device_id=device(z, y, 1 - core), device_id_type=MESH,
            )
            for i, (a, b) in enumerate(((k_hbm, kbuf), (v_hbm, vbuf)))
        )

    def self_remote():
        cols = pl.ds((1 - core) * half_kv, half_kv)
        return tuple(
            pltpu.make_async_remote_copy(
                a.at[:, cols], b.at[core], kv_send.at[i, CHUNKS], kv_recv.at[i, CHUNKS],
                device_id=device(z, y, 1 - core), device_id_type=MESH,
            )
            for i, (a, b) in enumerate(((qk_hbm, kself), (qv_hbm, vself)))
        )

    def q_piece(c, cc):
        return qown.at[:, pl.ds(cc * half_q + c * q_wide, q_wide)]

    def zq(c, zz, cc):
        return pltpu.make_async_remote_copy(
            q_piece(c, cc), qbuf.at[c, y, z, core], zq_send.at[c, zz, cc], zq_recv.at[c, z, core],
            device_id=device(zz, y, cc), device_id_type=MESH,
        )

    def zq_wait(c, zz):
        for cc in range(2):
            pltpu.make_async_remote_copy(
                q_piece(c, cc), qbuf.at[c, y, zz, cc], zq_send.at[c, zz, cc], zq_recv.at[c, zz, cc],
                device_id=device(zz, y, cc), device_id_type=MESH,
            ).wait_recv()

    def yq(c, cc):
        return pltpu.make_async_remote_copy(
            q_piece(c, cc), qbuf.at[c, y, z, core], yq_send.at[c, cc], yq_recv.at[c, core],
            device_id=device(z, 1 - y, cc), device_id_type=MESH,
        )

    def yq_wait(c):
        for cc in range(2):
            pltpu.make_async_remote_copy(
                q_piece(c, cc), qbuf.at[c, 1 - y, z, cc], yq_send.at[c, cc], yq_recv.at[c, cc],
                device_id=device(z, 1 - y, cc), device_id_type=MESH,
            ).wait_recv()

    def pq(c):
        return pltpu.make_async_remote_copy(
            q_piece(c, 1 - core), qbuf.at[c, y, z, core], pq_send.at[c], pq_recv.at[c],
            device_id=device(z, y, 1 - core), device_id_type=MESH,
        )

    def forward(c, zz):
        return pltpu.make_async_remote_copy(
            qbuf.at[c, y, zz], qbuf.at[c, y, zz], f_send.at[c, zz], f_recv.at[c, zz],
            device_id=device(z, 1 - y, core), device_id_type=MESH,
        )

    def p_copy(c):
        return pltpu.make_async_remote_copy(
            nsend.at[c], narr.at[c], p_send.at[c], p_recv.at[c],
            device_id=device(z, 1 - y, core), device_id_type=MESH,
        )

    def w_copy(c, zz):
        return pltpu.make_async_remote_copy(
            wsend.at[c, zz], warr.at[c, z], w_send.at[c, zz], w_recv.at[c, z],
            device_id=device(zz, y, core), device_id_type=MESH,
        )

    def w_wait(c, zz):
        pltpu.make_async_remote_copy(
            wsend.at[c, zz], warr.at[c, zz], w_send.at[c, zz], w_recv.at[c, zz],
            device_id=device(zz, y, core), device_id_type=MESH,
        ).wait_recv()

    def o_copy(c):
        return pltpu.make_async_remote_copy(
            osend.at[c], o_ref.at[:, pl.ds(core * half_q + c * wide, wide)], o_send.at[c], o_recv.at[c],
            device_id=device(z, y, 1 - core), device_id_type=MESH,
        )

    for c in range(PIECES):
        q_own(c).start()
    for c in range(CHUNKS):
        for copy in reversed(kv_local(c)):
            copy.start()
    with jax.named_scope("enter"):
        q_in.wait()
        pl.semaphore_wait(barrier, len(peers))

    for c in range(PIECES):
        for zz in reversed(others):
            for cc in range(2):
                zq(c, zz, cc).start()
        for cc in range(2):
            yq(c, cc).start()
        pq(c).start()
        if c == 0:
            for copy in self_remote():
                copy.start()
    for c in range(CHUNKS):
        for copy in reversed(kv_remote(c)):
            copy.start()

    for copy in small:
        copy.wait()
    place = chip * docs + lax.broadcasted_iota(jnp.int32, (docs, LANE), 0)
    bias_doc[...] = jnp.where(place < off_ref[0], 0.0, MASKED)
    spot = lax.broadcasted_iota(jnp.int32, (selves, 2 * LANE), 1)
    key_row = chip * selves + lax.broadcasted_iota(jnp.int32, (selves, 2 * LANE), 0)
    inner = spot % side
    row = ((inner // (2 * rows)) * 2 + jnp.where(spot < LANE, y, 1 - y)) * (2 * rows) + inner % (2 * rows)
    bias_self[...] = jnp.where(key_row <= row, 0.0, MASKED)
    ones = lax.broadcasted_iota(jnp.int32, (16, docs + LANE), 0) == 0
    ones = jnp.where(ones, 1.0, 0.0).astype(vt.dtype)
    for g in range(HALF_KVH):
        vt[g, HD:, :] = ones
    for copy in self_remote():
        copy.wait_recv()
    kbuf[docs:, :] = kself[...].astype(jnp.float32).reshape(selves, half_kv).astype(kbuf.dtype)
    vbuf[docs:, :] = vself[...].astype(jnp.float32).reshape(selves, half_kv).astype(kbuf.dtype)

    def turn(c):
        with jax.named_scope("kv"):
            for copy in kv_local(c):
                copy.wait()
            for copy in kv_remote(c):
                copy.wait_recv()
        for g in range(GROUPS):
            cols = slice((c * GROUPS + g) * HD, (c * GROUPS + g + 1) * HD)
            vt[c * GROUPS + g, :HD, :docs] = vbuf[:docs, cols].T
            last = vbuf[docs:, cols].astype(jnp.float32)
            last = jnp.concatenate([last, jnp.zeros((LANE - selves, HD), jnp.float32)], axis=0)
            vt[c * GROUPS + g, :HD, docs:] = last.T.astype(vt.dtype)

    def relay(c):
        for zz in others:
            zq_wait(c, zz)
            forward(c, zz).start()

    factor = QSCALE ** (-0.5) * LOG2E
    tile = 256
    per_piece = CHUNKS // PIECES

    def attend(c):
        piece = c // per_piece
        if c % per_piece == 0:
            with jax.named_scope("queries"):
                q_own(piece).wait()
                pq(piece).wait_recv()
                yq_wait(piece)
                for zz in others:
                    forward(piece, zz).wait_recv()
        for g in range(GROUPS):
            at = c * GROUPS + g
            cols = slice(at * HD, (at + 1) * HD)
            pieces = []
            for yy in (y, 1 - y):
                for j in range(PER_GROUP):
                    h = ((c % per_piece) * GROUPS + g) * PER_GROUP + j
                    block = qbuf[piece, yy, :, :, :, h * HD : (h + 1) * HD].astype(jnp.float32)
                    pieces.append(block.reshape(side, HD).astype(jnp.bfloat16))
            query = jnp.concatenate(pieces, axis=0)
            top = None
            for start in list(range(0, docs, tile)) + [docs]:
                size = tile if start < docs else selves
                part = lax.dot_general(
                    kbuf[start : start + size, cols], query, (((1,), (1,)), ((), ())),
                    preferred_element_type=jnp.float32,
                )
                if start < docs:
                    mask = bias_doc[start : start + size, :]
                    part = part + jnp.concatenate([mask, mask], axis=1)
                else:
                    part = part + bias_self[...]
                scores[at % 2, start : start + size, :] = part
                most = jnp.max(part.reshape(size // 8, 8, 2 * LANE), axis=0)
                top = most if top is None else jnp.maximum(top, most)
            top = jnp.max(top, axis=0, keepdims=True)
            total = None
            for start in list(range(0, docs, tile)) + [docs]:
                size = tile if start < docs else selves
                part = scores[at % 2, start : start + size, :]
                weights = jnp.exp2((part - top) * factor)
                span = size
                if start == docs:
                    span = LANE
                    weights = jnp.concatenate(
                        [weights, jnp.zeros((LANE - selves, 2 * LANE), jnp.float32)], axis=0
                    )
                got = jnp.dot(
                    vt[at, :, start : start + span], weights.astype(jnp.bfloat16),
                    preferred_element_type=jnp.float32,
                )
                total = got if total is None else total + got
            top = top * factor
            den = total[HD : HD + 1]
            num = total[:HD]
            nkeep[c, g * HD : (g + 1) * HD, :] = num[:, :LANE]
            skeep[c, 2 * g : 2 * g + 1, :] = top[:, :LANE]
            skeep[c, 2 * g + 1 : 2 * g + 2, :] = den[:, :LANE]
            out = num[:, LANE:]
            largest = jnp.maximum(jnp.max(jnp.abs(out), axis=0, keepdims=True), 1e-30)
            nsend[c, g * HD : (g + 1) * HD, :] = encode(out * (WIRE_TOP / largest))
            skeep[c, 4 + g : 5 + g, :] = top[:, LANE:] + log2(den[:, LANE:])
            skeep[c, 6 + g : 7 + g, :] = top[:, LANE:] + log2(largest)
        logs = split(skeep[c, 4:8, :])
        logs = jnp.concatenate([logs, jnp.zeros((8, LANE), jnp.float32)], axis=0)
        nsend[c, GROUPS * HD :, :] = encode(logs)
        p_copy(c).start()

    def pair_up(c):
        with jax.named_scope("pair"):
            p_copy(c).wait_recv()
        logs = decode(narr[c, GROUPS * HD :, :])
        logs = logs[:4] * COARSE + logs[4:8] * FINE
        mass, span = [], []
        for g in range(GROUPS):
            top_a, den_a = skeep[c, 2 * g : 2 * g + 1, :], skeep[c, 2 * g + 1 : 2 * g + 2, :]
            mass_b, span_b = logs[g : g + 1], logs[2 + g : 3 + g]
            top = jnp.maximum(top_a, mass_b)
            fa = jnp.exp2(top_a - top)
            den = den_a * fa + jnp.exp2(mass_b - top)
            fb = jnp.exp2(span_b - top) * (1.0 / WIRE_TOP)
            at = slice(g * HD, (g + 1) * HD)
            num = nkeep[c, at, :] * fa + decode(narr[c, at, :]) * fb
            largest = jnp.maximum(jnp.max(jnp.abs(num), axis=0, keepdims=True), 1e-30)
            codes = encode((num * (WIRE_TOP / largest)).T)
            for j in range(PER_GROUP):
                h = g * PER_GROUP + j
                wsend[c, :, :, h * HD : (h + 1) * HD] = codes[j * side : (j + 1) * side].reshape(
                    length, 2 * rows, HD
                )
            mass.append(top + log2(den))
            span.append(top + log2(largest))
        table = split(jnp.concatenate(mass + span, axis=0))
        table = jnp.concatenate([table, jnp.zeros((LANE - 8, LANE), jnp.float32)], axis=0)
        table = encode(table.T)
        for j in range(PER_GROUP):
            wsend[c, :, :, wide + 8 * j : wide + 8 * j + 8] = table[j * side : (j + 1) * side, :8].reshape(
                length, 2 * rows, 8
            )
        for zz in reversed(others):
            w_copy(c, zz).start()
        warr[c, z] = wsend[c, z]

    def finish(c):
        with jax.named_scope("parts"):
            for zz in others:
                w_wait(c, zz)
        logs = []
        for k in range(length):
            block = decode(warr[c, k, :, wide:])
            logs.append(block * COARSE + pltpu.roll(block, LANE - 4, 1) * FINE)
        most = functools.reduce(jnp.maximum, logs)
        den = sum(jnp.exp2(x - most) for x in logs)
        most, den = pltpu.roll(most, 2, 1), pltpu.roll(den, 2, 1)
        share = 1.0 / (den * WIRE_TOP)
        coefs = [jnp.exp2(x - most) * share for x in logs]
        mine = chip * selves + lax.broadcasted_iota(jnp.int32, (selves, HD), 0)
        live = mine < len_ref[0]
        for g in range(GROUPS):
            for j in range(PER_GROUP):
                h = g * PER_GROUP + j
                at = 8 * j + 2 + g
                acc = None
                for k in range(length):
                    term = decode(warr[c, k, :, h * HD : (h + 1) * HD]) * coefs[k][:, at : at + 1]
                    acc = term if acc is None else acc + term
                acc = jnp.where(live, acc, 0.0)
                kept = jnp.where(core == 0, acc[:rows], acc[rows:])
                sent = jnp.where(core == 0, acc[rows:], acc[:rows])
                to = pl.multiple_of(core * half_q + c * wide + h * HD, HD)
                o_ref[:, pl.ds(to, HD)] = kept.astype(o_ref.dtype)
                osend[c, :, h * HD : (h + 1) * HD] = sent.astype(o_ref.dtype)
        o_copy(c).start()

    def drain():
        for copy in self_remote():
            copy.wait_send()
        for c in range(CHUNKS):
            for copy in kv_remote(c):
                copy.wait_send()
        for c in range(PIECES):
            pq(c).wait_send()
            for cc in range(2):
                yq(c, cc).wait_send()
            for zz in others:
                forward(c, zz).wait_send()
                for cc in range(2):
                    zq(c, zz, cc).wait_send()
        for c in range(CHUNKS):
            p_copy(c).wait_send()

    def run(name, step, c):
        with jax.named_scope(f"{name}#c={c}"):
            step(c)

    run("relay", relay, 0)
    run("turn", turn, 0)
    run("turn", turn, 1)
    run("relay", relay, 1)
    for c in range(CHUNKS):
        run("attend", attend, c)
        if c + 2 < CHUNKS:
            run("turn", turn, c + 2)
        if c > 0:
            run("pair_up", pair_up, c - 1)
    run("pair_up", pair_up, CHUNKS - 1)
    with jax.named_scope("drain"):
        drain()
    for c in range(CHUNKS):
        run("finish", finish, c)
    with jax.named_scope("last"):
        for c in range(CHUNKS):
            for zz in others:
                w_copy(c, zz).wait_send()
            o_copy(c).wait_send()
        for c in range(CHUNKS):
            pltpu.make_async_remote_copy(
                osend.at[c], o_ref.at[:, pl.ds((1 - core) * half_q + c * wide, wide)],
                o_send.at[c], o_recv.at[c], device_id=device(z, y, 1 - core), device_id_type=MESH,
            ).wait_recv()


COARSE = 2.0 ** -5
FINE = 2.0 ** -20


def split(x):
    x = jnp.maximum(x, -1000.0)
    high = jnp.round(x * (1.0 / COARSE))
    return jnp.concatenate([high, (x - high * COARSE) * (1.0 / FINE)], axis=0)


def log2(x):
    return jnp.log(x) * LOG2E


def encode(x):
    return jnp.round(x).astype(jnp.int32).astype(WIRE)


def decode(x):
    return x.astype(jnp.int32).astype(jnp.float32)


def fused(n, queries, question_keys, question_values, doc_keys, doc_values, lengths, offsets):
    rows = queries.shape[0]
    doc = doc_keys.shape[0]
    if (
        NQ != 1 or n != 16 or rows % 8 or n * rows * PER_GROUP != 2 * LANE
        or doc % LANE or doc > 1024 or n * rows != QL
    ):
        return local(
            queries, question_keys, question_values, doc_keys, doc_values, lengths, offsets
        )
    operands = (queries, question_keys, question_values, doc_keys, doc_values)
    length = n // 4
    docs, selves = 2 * doc, 2 * rows
    half_kv = HALF_KVH * HD
    wide = GROUPS * PER_GROUP * HD
    q_wide = half_kv * PER_GROUP // PIECES
    vmem = pl.BlockSpec(memory_space=pltpu.VMEM)
    hbm = pl.BlockSpec(memory_space=pltpu.HBM)
    smem = pl.BlockSpec(memory_space=pltpu.SMEM)
    f32, bf16 = jnp.float32, jnp.bfloat16
    dma = pltpu.SemaphoreType.DMA
    return pl.pallas_call(
        functools.partial(fused_kernel, n),
        out_shape=jax.ShapeDtypeStruct(queries.shape, bf16),
        in_specs=[hbm] * 5 + [smem] * 2,
        out_specs=vmem,
        scratch_shapes=[
            pltpu.VMEM((rows, H * HD), bf16),
            pltpu.VMEM((PIECES, 2, length, 2, rows, q_wide), bf16),
            pltpu.VMEM((2, rows, half_kv), bf16),
            pltpu.VMEM((2, rows, half_kv), bf16),
            pltpu.VMEM((docs + selves, half_kv), bf16),
            pltpu.VMEM((HALF_KVH, HD + 16, docs + LANE), bf16),
            pltpu.VMEM((docs, LANE), f32),
            pltpu.VMEM((selves, 2 * LANE), f32),
            pltpu.VMEM((2, docs + selves, 2 * LANE), f32),
            pltpu.VMEM((docs + selves, half_kv), bf16),
            pltpu.VMEM((CHUNKS, GROUPS * HD, LANE), f32),
            pltpu.VMEM((CHUNKS, STATS, LANE), f32),
            pltpu.VMEM((CHUNKS, GROUPS * HD + 16, LANE), WIRE),
            pltpu.VMEM((CHUNKS, GROUPS * HD + 16, LANE), WIRE),
            pltpu.VMEM((CHUNKS, length, 2 * rows, wide + LANE), WIRE),
            pltpu.VMEM((CHUNKS, length, 2 * rows, wide + LANE), WIRE),
            pltpu.VMEM((CHUNKS, rows, wide), bf16),
            dma((PIECES + 1,)),
            dma((2,)),
            dma((2, CHUNKS)),
            dma((2, CHUNKS + 1)),
            dma((2, CHUNKS + 1)),
            dma((PIECES, length, 2)),
            dma((PIECES, length, 2)),
            dma((PIECES, 2)),
            dma((PIECES, 2)),
            dma((PIECES,)),
            dma((PIECES,)),
            dma((PIECES, length)),
            dma((PIECES, length)),
            dma((CHUNKS,)),
            dma((CHUNKS,)),
            dma((CHUNKS, length)),
            dma((CHUNKS, length)),
            dma((CHUNKS,)),
            dma((CHUNKS,)),
        ],
        compiler_params=pltpu.CompilerParams(
            collective_id=0, has_side_effects=True, vmem_limit_bytes=24 * 1024 * 1024
        ),
    )(*(pltpu.with_memory_space_constraint(x, pltpu.HBM) for x in operands), lengths, offsets)


def solution(mesh):
    placed = (
        P(("grp", "seq"), None),
        P(("grp", "seq"), None),
        P(("grp", "seq"), None),
        P(("grp", "seq"), None),
        P(("grp", "seq"), None),
        P("grp"),
        P("grp"),
    )
    return jax.shard_map(
        functools.partial(fused, mesh.shape["seq"]),
        mesh=mesh, in_specs=placed, out_specs=P(("grp", "seq"), None), check_vma=False,
    )
```

```python
import functools
import math

import jax
import jax.numpy as jnp
from jax import lax
from jax.experimental import pallas as pl
from jax.experimental.pallas import tpu as pltpu
from jax.sharding import PartitionSpec as P

H = 32
KVH = 16
HD = 128
QSCALE = 144
QL = 128
NQ = 1


MASKED = -1e30


def row_tables(start, count, lengths, offsets):
    rows = start + jnp.arange(count, dtype=jnp.int32)
    question = rows // QL
    position = rows % QL
    owner_table = question[:, None] == jnp.arange(NQ, dtype=jnp.int32)[None, :]
    row_length = jnp.sum(jnp.where(owner_table, lengths[None, :], 0), axis=1)
    row_offset = jnp.sum(jnp.where(owner_table, offsets[None, :], 0), axis=1)
    return (question, position, position < row_length, row_offset)


def local(queries, question_keys, question_values, doc_keys, doc_values, lengths, offsets):
    rows_local = queries.shape[0]
    doc_local = doc_keys.shape[0]
    device_count = lax.axis_size("seq")
    device_index = lax.axis_index("seq")
    total_rows = rows_local * device_count
    per_group = H // KVH
    factor_q = QSCALE ** (-0.5)
    key_doc = doc_keys.reshape(doc_local, KVH, HD)
    value_doc = doc_values.reshape(doc_local, KVH, HD)
    key_self = question_keys.reshape(rows_local, KVH, HD)
    value_self = question_values.reshape(rows_local, KVH, HD)
    doc_places = device_index * doc_local + jnp.arange(doc_local, dtype=jnp.int32)
    self_rows = device_index * rows_local + jnp.arange(rows_local, dtype=jnp.int32)
    whole = lax.all_gather(queries, "seq", axis=0, tiled=True)
    block_rows = math.gcd(total_rows, 512)
    block_count = total_rows // block_rows

    def one_block(start):
        piece = whole.reshape(block_rows, KVH, per_group, HD)
        question, position, live_rows, row_offset = row_tables(start, block_rows, lengths, offsets)
        mask_doc = live_rows[:, None] & (doc_places[None, :] < row_offset[:, None])
        mask_self = (
            live_rows[:, None]
            & (self_rows[None, :] // QL == question[:, None])
            & (self_rows[None, :] % QL <= position[:, None])
        )
        mask_doc = mask_doc[:, None, None, :]
        mask_self = mask_self[:, None, None, :]
        scores_doc = (
            jnp.einsum("rgjd,kgd->rgjk", piece, key_doc, preferred_element_type=jnp.float32)
            * factor_q
        )
        scores_self = (
            jnp.einsum("rgjd,kgd->rgjk", piece, key_self, preferred_element_type=jnp.float32)
            * factor_q
        )
        scores_doc = jnp.where(mask_doc, scores_doc, MASKED)
        scores_self = jnp.where(mask_self, scores_self, MASKED)
        block_top = jnp.maximum(jnp.max(scores_doc, axis=-1), jnp.max(scores_self, axis=-1))
        weights_doc = jnp.where(mask_doc, jnp.exp(scores_doc - block_top[..., None]), 0.0).astype(
            jnp.bfloat16
        )
        weights_self = jnp.where(
            mask_self, jnp.exp(scores_self - block_top[..., None]), 0.0
        ).astype(jnp.bfloat16)
        block_den = jnp.sum(weights_doc.astype(jnp.float32), axis=-1) + jnp.sum(
            weights_self.astype(jnp.float32), axis=-1
        )
        block_num = jnp.einsum(
            "rgjk,kgd->rgjd", weights_doc, value_doc, preferred_element_type=jnp.float32
        )
        block_num = block_num + jnp.einsum(
            "rgjk,kgd->rgjd", weights_self, value_self, preferred_element_type=jnp.float32
        )
        return (
            block_num.reshape(block_rows, H * HD),
            block_top.reshape(block_rows, H),
            block_den.reshape(block_rows, H),
        )

    starts = jnp.arange(block_count, dtype=jnp.int32) * block_rows
    numer, row_top, denom = lax.map(one_block, starts)
    numer = numer.reshape(total_rows, H * HD)
    row_top = row_top.reshape(total_rows, H)
    denom = denom.reshape(total_rows, H)
    got_num, got_top, got_den = (
        lax.all_to_all(numer[None], "seq", split_axis=1, concat_axis=0, tiled=True),
        lax.all_to_all(row_top[None], "seq", split_axis=1, concat_axis=0, tiled=True),
        lax.all_to_all(denom[None], "seq", split_axis=1, concat_axis=0, tiled=True),
    )
    overall = jnp.max(got_top, axis=0)
    rescale = jnp.exp(got_top - overall[None])
    total_num = jnp.sum(
        got_num.reshape(device_count, rows_local, H, HD) * rescale[:, :, :, None], axis=0
    )
    total_den = jnp.sum(got_den * rescale, axis=0)
    question, position, live_rows, row_offset = row_tables(
        device_index * rows_local, rows_local, lengths, offsets
    )
    safe_den = jnp.where(live_rows[:, None], total_den, 1.0)
    result = (total_num / safe_den[:, :, None]).reshape(rows_local, H * HD)
    return jnp.where(live_rows[:, None], result, 0.0).astype(jnp.bfloat16)


MESH = pl.DeviceIdType.MESH
LANE = 128
CHUNKS = 4
PIECES = ((0, 1), (1, 4))
WHOLE = (0, 4)
LOG2E = math.log2(math.e)
WIRE = jnp.int16
WIRE_TOP = 32767.0
HALF_KVH = KVH // 2
PER_GROUP = H // KVH
GROUPS = HALF_KVH // CHUNKS
STATS = 8
QK_TILE = 256
AHEAD = True


def fused_kernel(
    n, q_hbm, qk_hbm, qv_hbm, k_hbm, v_hbm, len_ref, off_ref, o_ref,
    qown, qbuf, kself, vself, kbuf, vt, key_mask, row_mask, scores, probs, vbuf,
    nkeep, skeep, nsend, narr, wsend, warr, osend,
    q_sem, in_sem, kv_sem, kv_send, kv_recv,
    zq_send, zq_recv, yq_send, yq_recv, pq_recv, f_send, f_recv, far,
    p_send, p_recv, w_send, w_recv, o_send, o_recv,
):
    length = n // 4
    rows = q_hbm.shape[0]
    doc = k_hbm.shape[0]
    docs = 2 * doc
    selves = 2 * rows
    half_kv = HALF_KVH * HD
    half_q = half_kv * PER_GROUP
    kv_wide = GROUPS * HD
    wide = kv_wide * PER_GROUP
    side = length * 2 * rows
    me = lax.axis_index("seq")
    core = lax.rem(me, 2)
    chip = me // 2
    y = lax.rem(chip, 2)
    z = chip // 2
    others = (z + 1 - 2 * lax.rem(z, 2), 2 - z // 2, 3 - 3 * (z // 2))

    def device(zz, yy, cc):
        return {"seq": (zz * 2 + yy) * 2 + cc}

    middle = (lax.rem(z, length - 1) + 1) // 2
    across = 1 + lax.rem(z, 2)
    near = others[0]
    barrier = pltpu.get_barrier_semaphore()
    peers = [device(z, y, 1 - core)] + [device(z, 1 - y, cc) for cc in range(2)]
    peers += [device(near, y, cc) for cc in range(2)]
    for peer in peers:
        pl.semaphore_signal(barrier, inc=1, device_id=peer, device_id_type=MESH)

    @pl.when(middle == 1)
    def greet():
        for cc in range(2):
            pl.semaphore_signal(barrier, inc=1, device_id=device(across, y, cc), device_id_type=MESH)

    q_in = pltpu.make_async_copy(q_hbm, qown, q_sem.at[1])
    q_in.start()
    small = [
        pltpu.make_async_copy(qk_hbm.at[:, pl.ds(core * half_kv, half_kv)], kself.at[core], in_sem.at[0]),
        pltpu.make_async_copy(qv_hbm.at[:, pl.ds(core * half_kv, half_kv)], vself.at[core], in_sem.at[1]),
    ]
    for copy in small:
        copy.start()

    def part(piece):
        return pl.ds(piece[0] * wide, (piece[1] - piece[0]) * wide)

    q_own = pltpu.make_async_copy(q_hbm.at[:, pl.ds(core * half_q, half_q)], qbuf.at[y, z, core], q_sem.at[0])

    def kv_local(c):
        cols = pl.ds(core * half_kv + c * kv_wide, kv_wide)
        at = pl.ds(core * doc, doc)
        to = pl.ds(c * kv_wide, kv_wide)
        return (
            pltpu.make_async_copy(k_hbm.at[:, cols], kbuf.at[at, to], kv_sem.at[0, c]),
            pltpu.make_async_copy(v_hbm.at[:, cols], vbuf.at[at, to], kv_sem.at[1, c]),
        )

    def kv_remote(c):
        cols = pl.ds((1 - core) * half_kv + c * kv_wide, kv_wide)
        at = pl.ds(core * doc, doc)
        to = pl.ds(c * kv_wide, kv_wide)
        return tuple(
            pltpu.make_async_remote_copy(
                a.at[:, cols], b.at[at, to], kv_send.at[i, c], kv_recv.at[i, c],
                device_id=device(z, y, 1 - core), device_id_type=MESH,
            )
            for i, (a, b) in enumerate(((k_hbm, kbuf), (v_hbm, vbuf)))
        )

    def self_remote():
        cols = pl.ds((1 - core) * half_kv, half_kv)
        return tuple(
            pltpu.make_async_remote_copy(
                a.at[:, cols], b.at[core], kv_send.at[i, CHUNKS], kv_recv.at[i, CHUNKS],
                device_id=device(z, y, 1 - core), device_id_type=MESH,
            )
            for i, (a, b) in enumerate(((qk_hbm, kself), (qv_hbm, vself)))
        )

    def q_copy(where, i, piece, send_sem, recv_sem):
        zz, yy, cc = where
        return pltpu.make_async_remote_copy(
            qown.at[:, pl.ds(cc * half_q + piece[0] * wide, (piece[1] - piece[0]) * wide)],
            qbuf.at[y, z, core, :, part(piece)], send_sem.at[i, zz, cc], recv_sem.at[i, z, core],
            device_id=device(zz, yy, cc), device_id_type=MESH,
        )

    def q_wait(where, i, piece, send_sem, recv_sem):
        zz, yy, cc = where
        pltpu.make_async_remote_copy(
            qown.at[:, part(piece)], qbuf.at[yy, zz, cc, :, part(piece)],
            send_sem.at[i, zz, cc], recv_sem.at[i, zz, cc],
            device_id=device(zz, yy, cc), device_id_type=MESH,
        ).wait_recv()

    def pieces(order):
        return enumerate((WHOLE,) if order == 0 else PIECES)

    def zq(order, i, piece, cc):
        return q_copy((others[order], y, cc), i, piece, zq_send, zq_recv)

    def yq(cc):
        return q_copy((z, 1 - y, cc), 0, WHOLE, yq_send, yq_recv)

    def pq():
        return q_copy((z, y, 1 - core), 0, WHOLE, yq_send, pq_recv)

    def forward(order, i, piece):
        zz = others[order]
        return pltpu.make_async_remote_copy(
            qbuf.at[y, zz, :, :, part(piece)], qbuf.at[y, zz, :, :, part(piece)],
            f_send.at[i, zz], f_recv.at[i, zz],
            device_id=device(z, 1 - y, core), device_id_type=MESH,
        )

    def p_copy(c):
        return pltpu.make_async_remote_copy(
            nsend.at[c], narr.at[c], p_send.at[c], p_recv.at[c],
            device_id=device(z, 1 - y, core), device_id_type=MESH,
        )

    def w_copy(c, zz):
        return pltpu.make_async_remote_copy(
            wsend.at[c, zz], warr.at[c, z], w_send.at[c, zz], w_recv.at[c, z],
            device_id=device(zz, y, core), device_id_type=MESH,
        )

    def w_wait(c, zz):
        pltpu.make_async_remote_copy(
            wsend.at[c, zz], warr.at[c, zz], w_send.at[c, zz], w_recv.at[c, zz],
            device_id=device(zz, y, core), device_id_type=MESH,
        ).wait_recv()

    def o_copy(c):
        return pltpu.make_async_remote_copy(
            osend.at[c], o_ref.at[:, pl.ds(core * half_q + c * wide, wide)], o_send.at[c], o_recv.at[c],
            device_id=device(z, y, 1 - core), device_id_type=MESH,
        )

    q_own.start()
    for c in range(CHUNKS):
        for copy in reversed(kv_local(c)):
            copy.start()
    with jax.named_scope("enter"):
        q_in.wait()
        pl.semaphore_wait(barrier, len(peers) + 2 * middle)

    @pl.when(middle == 1)
    def spread():
        pl.semaphore_signal(far.at[0], inc=1, device_id=device(near, y, core), device_id_type=MESH)
        pl.semaphore_signal(far.at[1], inc=1, device_id=device(across, y, core), device_id_type=MESH)

    for cc in range(2):
        yq(cc).start()
    for cc in range(2):
        zq(0, 0, WHOLE, cc).start()
    pq().start()
    for copy in self_remote():
        copy.start()
    for c in range(CHUNKS):
        for copy in reversed(kv_remote(c)):
            copy.start()
    for order in (1, 2):
        if order == 1:

            @pl.when(middle == 0)
            def await_second():
                pl.semaphore_wait(far.at[0], 1)
        else:
            pl.semaphore_wait(far.at[1], 1)

            @pl.when(middle == 1)
            def pass_on():
                pl.semaphore_signal(far.at[1], inc=1, device_id=device(near, y, core), device_id_type=MESH)

        for i, piece in pieces(order):
            for cc in range(2):
                zq(order, i, piece, cc).start()

    for copy in small:
        copy.wait()
    place = lax.broadcasted_iota(jnp.int32, (docs, LANE), 0)
    lane = lax.broadcasted_iota(jnp.int32, (docs, LANE), 1)
    hidden = (chip * docs + place >= off_ref[0]) & (lane == 0)
    key_mask[:docs, :] = jnp.where(hidden, MASKED, 0.0).astype(key_mask.dtype)
    own = lane[:selves] == place[:selves] + 1
    key_mask[docs:, :] = jnp.where(own, 1.0, 0.0).astype(key_mask.dtype)
    spot, lane = place[: 2 * LANE], lane[: 2 * LANE]
    inner = spot % side
    row = ((inner // (2 * rows)) * 2 + jnp.where(spot < LANE, y, 1 - y)) * (2 * rows) + inner % (2 * rows)
    later = (lane <= selves) & (chip * selves + lane - 1 > row)
    row_mask[...] = jnp.where(lane == 0, 1.0, jnp.where(later, MASKED, 0.0)).astype(row_mask.dtype)
    ones = lax.broadcasted_iota(jnp.int32, (16, docs + LANE), 0) == 0
    ones = jnp.where(ones, 1.0, 0.0).astype(vt.dtype)
    for g in range(HALF_KVH):
        vt[g, HD:, :] = ones
    for copy in self_remote():
        copy.wait_recv()
    kbuf[docs:, :] = kself[...].astype(jnp.float32).reshape(selves, half_kv).astype(kbuf.dtype)
    vbuf[docs:, :] = vself[...].astype(jnp.float32).reshape(selves, half_kv).astype(kbuf.dtype)

    def turn(c):
        with jax.named_scope("kv"):
            for copy in kv_local(c):
                copy.wait()
            for copy in kv_remote(c):
                copy.wait_recv()
        for g in range(GROUPS):
            cols = slice((c * GROUPS + g) * HD, (c * GROUPS + g + 1) * HD)
            vt[c * GROUPS + g, :HD, :docs] = vbuf[:docs, cols].T
            last = vbuf[docs:, cols].astype(jnp.float32)
            last = jnp.concatenate([last, jnp.zeros((LANE - selves, HD), jnp.float32)], axis=0)
            vt[c * GROUPS + g, :HD, docs:] = last.T.astype(vt.dtype)

    def relay(c):
        for order in range(3):
            for i, piece in pieces(order):
                if i == c:
                    for cc in range(2):
                        q_wait((others[order], y, cc), i, piece, zq_send, zq_recv)
                    forward(order, i, piece).start()

    factor = QSCALE ** (-0.5) * LOG2E
    base = me // n
    tile = 256

    def attend(c):
        with jax.named_scope("queries"):
            if c == 0:
                q_own.wait()
                q_wait((z, y, 1 - core), 0, WHOLE, yq_send, pq_recv)
                for cc in range(2):
                    q_wait((z, 1 - y, cc), 0, WHOLE, yq_send, yq_recv)
            for order in range(3):
                for i, piece in pieces(order):
                    if piece[0] == c:
                        forward(order, i, piece).wait_recv()

        def load(g):
            pieces = []
            for yy in (y, 1 - y):
                for j in range(PER_GROUP):
                    h = (c * GROUPS + g) * PER_GROUP + j
                    block = qbuf[yy, :, :, :, h * HD : (h + 1) * HD].astype(jnp.float32)
                    pieces.append(block.reshape(side, HD).astype(jnp.bfloat16))
            return jnp.concatenate([jnp.concatenate(pieces, axis=0), row_mask[...]], axis=1)

        starts = list(range(0, docs, tile)) + [docs]
        q_starts = list(range(0, docs, QK_TILE)) + [docs]

        def score(g, query, start, top):
            at = c * GROUPS + g
            size = QK_TILE if start < docs else selves
            span = slice(start, start + size)
            key = jnp.concatenate([kbuf[span, at * HD : (at + 1) * HD], key_mask[span, :]], axis=1)
            part = lax.dot_general(
                key, query, (((1,), (1,)), ((), ())), preferred_element_type=jnp.float32
            )
            scores[base, at % 2, start : start + size, :] = part
            most = jnp.max(part.reshape(size // 8, 8, 2 * LANE), axis=0)
            return most if top is None else jnp.maximum(top, most)

        def weigh(g, start, top, total):
            at = c * GROUPS + g
            size = span = tile if start < docs else selves
            weights = jnp.exp2((scores[base, at % 2, start : start + size, :] - top) * factor)
            if start == docs:
                span = LANE
                weights = jnp.concatenate(
                    [weights, jnp.zeros((LANE - selves, 2 * LANE), jnp.float32)], axis=0
                )
            got = jnp.dot(
                vt[at, :, start : start + span], weights.astype(jnp.bfloat16),
                preferred_element_type=jnp.float32,
            )
            return got if total is None else total + got

        def begin(g):
            query, after = load(g), None
            for start in q_starts:
                after = score(g, query, start, after)
            return after

        after = begin(0)
        for g in range(GROUPS):
            top, total = jnp.max(after, axis=0, keepdims=True), None
            if g + 1 < GROUPS and AHEAD:
                after = begin(g + 1)
            for start in starts:
                total = weigh(g, start, top, total)
            if g + 1 < GROUPS and not AHEAD:
                after = begin(g + 1)
            top = top * factor
            den = total[HD : HD + 1]
            num = total[:HD]
            nkeep[c, g * HD : (g + 1) * HD, :] = num[:, :LANE]
            skeep[c, 2 * g : 2 * g + 1, :] = top[:, :LANE]
            skeep[c, 2 * g + 1 : 2 * g + 2, :] = den[:, :LANE]
            out = num[:, LANE:]
            largest = jnp.maximum(jnp.max(jnp.abs(out), axis=0, keepdims=True), 1e-30)
            nsend[c, g * HD : (g + 1) * HD, :] = encode(out * (WIRE_TOP / largest))
            skeep[c, 4 + g : 5 + g, :] = top[:, LANE:] + log2(den[:, LANE:])
            skeep[c, 6 + g : 7 + g, :] = top[:, LANE:] + log2(largest)
        logs = split(skeep[c, 4:8, :])
        logs = jnp.concatenate([logs, jnp.zeros((8, LANE), jnp.float32)], axis=0)
        nsend[c, GROUPS * HD :, :] = encode(logs)
        p_copy(c).start()

    def pair_up(c):
        with jax.named_scope("pair"):
            p_copy(c).wait_recv()
        logs = decode(narr[c, GROUPS * HD :, :])
        logs = logs[:4] * COARSE + logs[4:8] * FINE
        mass, span = [], []
        for g in range(GROUPS):
            top_a, den_a = skeep[c, 2 * g : 2 * g + 1, :], skeep[c, 2 * g + 1 : 2 * g + 2, :]
            mass_b, span_b = logs[g : g + 1], logs[2 + g : 3 + g]
            top = jnp.maximum(top_a, mass_b)
            fa = jnp.exp2(top_a - top)
            den = den_a * fa + jnp.exp2(mass_b - top)
            fb = jnp.exp2(span_b - top) * (1.0 / WIRE_TOP)
            at = slice(g * HD, (g + 1) * HD)
            num = nkeep[c, at, :] * fa + decode(narr[c, at, :]) * fb
            largest = jnp.maximum(jnp.max(jnp.abs(num), axis=0, keepdims=True), 1e-30)
            codes = encode((num * (WIRE_TOP / largest)).T)
            for j in range(PER_GROUP):
                h = g * PER_GROUP + j
                wsend[c, :, :, h * HD : (h + 1) * HD] = codes[j * side : (j + 1) * side].reshape(
                    length, 2 * rows, HD
                )
            mass.append(top + log2(den))
            span.append(top + log2(largest))
        table = split(jnp.concatenate(mass + span, axis=0))
        table = jnp.concatenate([table, jnp.zeros((LANE - 8, LANE), jnp.float32)], axis=0)
        table = encode(table.T)
        for j in range(PER_GROUP):
            wsend[c, :, :, wide + 8 * j : wide + 8 * j + 8] = table[j * side : (j + 1) * side, :8].reshape(
                length, 2 * rows, 8
            )
        for zz in reversed(others):
            w_copy(c, zz).start()
        warr[c, z] = wsend[c, z]

    def finish(c):
        with jax.named_scope("parts"):
            for zz in others:
                w_wait(c, zz)
        logs = []
        for k in range(length):
            block = decode(warr[c, k, :, wide:])
            logs.append(block * COARSE + pltpu.roll(block, LANE - 4, 1) * FINE)
        most = functools.reduce(jnp.maximum, logs)
        den = sum(jnp.exp2(x - most) for x in logs)
        most, den = pltpu.roll(most, 2, 1), pltpu.roll(den, 2, 1)
        share = 1.0 / (den * WIRE_TOP)
        coefs = [jnp.exp2(x - most) * share for x in logs]
        mine = chip * selves + lax.broadcasted_iota(jnp.int32, (selves, HD), 0)
        live = mine < len_ref[0]
        for g in range(GROUPS):
            for j in range(PER_GROUP):
                h = g * PER_GROUP + j
                at = 8 * j + 2 + g
                acc = None
                for k in range(length):
                    term = decode(warr[c, k, :, h * HD : (h + 1) * HD]) * coefs[k][:, at : at + 1]
                    acc = term if acc is None else acc + term
                acc = jnp.where(live, acc, 0.0)
                kept = jnp.where(core == 0, acc[:rows], acc[rows:])
                sent = jnp.where(core == 0, acc[rows:], acc[:rows])
                to = pl.multiple_of(core * half_q + c * wide + h * HD, HD)
                o_ref[:, pl.ds(to, HD)] = kept.astype(o_ref.dtype)
                osend[c, :, h * HD : (h + 1) * HD] = sent.astype(o_ref.dtype)
        o_copy(c).start()

    def drain():
        for copy in self_remote():
            copy.wait_send()
        for c in range(CHUNKS):
            for copy in kv_remote(c):
                copy.wait_send()
        pq().wait_send()
        for cc in range(2):
            yq(cc).wait_send()
        for order in range(3):
            for i, piece in pieces(order):
                forward(order, i, piece).wait_send()
                for cc in range(2):
                    zq(order, i, piece, cc).wait_send()
        for c in range(CHUNKS):
            p_copy(c).wait_send()

    def run(name, step, c):
        with jax.named_scope(f"{name}#c={c}"):
            step(c)

    run("turn", turn, 0)
    run("relay", relay, 0)
    run("turn", turn, 1)
    run("turn", turn, 2)
    run("relay", relay, 1)
    run("turn", turn, 3)
    for c in range(CHUNKS):
        run("attend", attend, c)
        if c > 1:
            run("pair_up", pair_up, c - 2)
    run("pair_up", pair_up, CHUNKS - 2)
    run("pair_up", pair_up, CHUNKS - 1)
    with jax.named_scope("drain"):
        drain()
    for c in range(CHUNKS):
        run("finish", finish, c)
    with jax.named_scope("last"):
        for c in range(CHUNKS):
            for zz in others:
                w_copy(c, zz).wait_send()
            o_copy(c).wait_send()
        for c in range(CHUNKS):
            pltpu.make_async_remote_copy(
                osend.at[c], o_ref.at[:, pl.ds((1 - core) * half_q + c * wide, wide)],
                o_send.at[c], o_recv.at[c], device_id=device(z, y, 1 - core), device_id_type=MESH,
            ).wait_recv()


COARSE = 2.0 ** -5
FINE = 2.0 ** -20


def split(x):
    x = jnp.maximum(x, -1000.0)
    high = jnp.round(x * (1.0 / COARSE))
    return jnp.concatenate([high, (x - high * COARSE) * (1.0 / FINE)], axis=0)


def log2(x):
    return jnp.log(x) * LOG2E


def encode(x):
    return jnp.round(x).astype(jnp.int32).astype(WIRE)


def decode(x):
    return x.astype(jnp.int32).astype(jnp.float32)


def fused(n, queries, question_keys, question_values, doc_keys, doc_values, lengths, offsets):
    rows = queries.shape[0]
    doc = doc_keys.shape[0]
    if (
        NQ != 1 or n != 16 or rows % 8 or n * rows * PER_GROUP != 2 * LANE
        or doc % LANE or doc > 1024 or n * rows != QL
    ):
        return local(
            queries, question_keys, question_values, doc_keys, doc_values, lengths, offsets
        )
    operands = (queries, question_keys, question_values, doc_keys, doc_values)
    length = n // 4
    docs, selves = 2 * doc, 2 * rows
    half_kv = HALF_KVH * HD
    wide = GROUPS * PER_GROUP * HD
    vmem = pl.BlockSpec(memory_space=pltpu.VMEM)
    hbm = pl.BlockSpec(memory_space=pltpu.HBM)
    smem = pl.BlockSpec(memory_space=pltpu.SMEM)
    f32, bf16 = jnp.float32, jnp.bfloat16
    pieces = len(PIECES)
    dma = pltpu.SemaphoreType.DMA
    return pl.pallas_call(
        functools.partial(fused_kernel, n),
        out_shape=jax.ShapeDtypeStruct(queries.shape, bf16),
        in_specs=[hbm] * 5 + [smem] * 2,
        out_specs=vmem,
        scratch_shapes=[
            pltpu.VMEM((rows, H * HD), bf16),
            pltpu.VMEM((2, length, 2, rows, half_kv * PER_GROUP), bf16),
            pltpu.VMEM((2, rows, half_kv), bf16),
            pltpu.VMEM((2, rows, half_kv), bf16),
            pltpu.VMEM((docs + selves, half_kv), bf16),
            pltpu.VMEM((HALF_KVH, HD + 16, docs + LANE), bf16),
            pltpu.VMEM((docs + selves, LANE), bf16),
            pltpu.VMEM((2 * LANE, LANE), bf16),
            pltpu.VMEM((1, 2, docs + selves, 2 * LANE), f32),
            pltpu.VMEM((1, docs + LANE, 2 * LANE), bf16),
            pltpu.VMEM((docs + selves, half_kv), bf16),
            pltpu.VMEM((CHUNKS, GROUPS * HD, LANE), f32),
            pltpu.VMEM((CHUNKS, STATS, LANE), f32),
            pltpu.VMEM((CHUNKS, GROUPS * HD + 16, LANE), WIRE),
            pltpu.VMEM((CHUNKS, GROUPS * HD + 16, LANE), WIRE),
            pltpu.VMEM((CHUNKS, length, 2 * rows, wide + LANE), WIRE),
            pltpu.VMEM((CHUNKS, length, 2 * rows, wide + LANE), WIRE),
            pltpu.VMEM((CHUNKS, rows, wide), bf16),
            dma((2,)),
            dma((2,)),
            dma((2, CHUNKS)),
            dma((2, CHUNKS + 1)),
            dma((2, CHUNKS + 1)),
            dma((pieces, length, 2)),
            dma((pieces, length, 2)),
            dma((1, length, 2)),
            dma((1, length, 2)),
            dma((1, length, 2)),
            dma((pieces, length)),
            dma((pieces, length)),
            pltpu.SemaphoreType.REGULAR((2,)),
            dma((CHUNKS,)),
            dma((CHUNKS,)),
            dma((CHUNKS, length)),
            dma((CHUNKS, length)),
            dma((CHUNKS,)),
            dma((CHUNKS,)),
        ],
        compiler_params=pltpu.CompilerParams(
            collective_id=0, has_side_effects=True, vmem_limit_bytes=24 * 1024 * 1024
        ),
    )(*(pltpu.with_memory_space_constraint(x, pltpu.HBM) for x in operands), lengths, offsets)


def solution(mesh):
    placed = (
        P(("grp", "seq"), None),
        P(("grp", "seq"), None),
        P(("grp", "seq"), None),
        P(("grp", "seq"), None),
        P(("grp", "seq"), None),
        P("grp"),
        P("grp"),
    )
    return jax.shard_map(
        functools.partial(fused, mesh.shape["seq"]),
        mesh=mesh, in_specs=placed, out_specs=P(("grp", "seq"), None), check_vma=False,
    )
```

```python
import functools
import math

import jax
import jax.numpy as jnp
from jax import lax
from jax.experimental import pallas as pl
from jax.experimental.pallas import tpu as pltpu
from jax.sharding import PartitionSpec as P

H = 32
KVH = 16
HD = 128
QSCALE = 144
QL = 128
NQ = 1


MASKED = -1e30


def row_tables(start, count, lengths, offsets):
    rows = start + jnp.arange(count, dtype=jnp.int32)
    question = rows // QL
    position = rows % QL
    owner_table = question[:, None] == jnp.arange(NQ, dtype=jnp.int32)[None, :]
    row_length = jnp.sum(jnp.where(owner_table, lengths[None, :], 0), axis=1)
    row_offset = jnp.sum(jnp.where(owner_table, offsets[None, :], 0), axis=1)
    return (question, position, position < row_length, row_offset)


def local(queries, question_keys, question_values, doc_keys, doc_values, lengths, offsets):
    rows_local = queries.shape[0]
    doc_local = doc_keys.shape[0]
    device_count = lax.axis_size("seq")
    device_index = lax.axis_index("seq")
    total_rows = rows_local * device_count
    per_group = H // KVH
    factor_q = QSCALE ** (-0.5)
    key_doc = doc_keys.reshape(doc_local, KVH, HD)
    value_doc = doc_values.reshape(doc_local, KVH, HD)
    key_self = question_keys.reshape(rows_local, KVH, HD)
    value_self = question_values.reshape(rows_local, KVH, HD)
    doc_places = device_index * doc_local + jnp.arange(doc_local, dtype=jnp.int32)
    self_rows = device_index * rows_local + jnp.arange(rows_local, dtype=jnp.int32)
    whole = lax.all_gather(queries, "seq", axis=0, tiled=True)
    block_rows = math.gcd(total_rows, 512)
    block_count = total_rows // block_rows

    def one_block(start):
        piece = whole.reshape(block_rows, KVH, per_group, HD)
        question, position, live_rows, row_offset = row_tables(start, block_rows, lengths, offsets)
        mask_doc = live_rows[:, None] & (doc_places[None, :] < row_offset[:, None])
        mask_self = (
            live_rows[:, None]
            & (self_rows[None, :] // QL == question[:, None])
            & (self_rows[None, :] % QL <= position[:, None])
        )
        mask_doc = mask_doc[:, None, None, :]
        mask_self = mask_self[:, None, None, :]
        scores_doc = (
            jnp.einsum("rgjd,kgd->rgjk", piece, key_doc, preferred_element_type=jnp.float32)
            * factor_q
        )
        scores_self = (
            jnp.einsum("rgjd,kgd->rgjk", piece, key_self, preferred_element_type=jnp.float32)
            * factor_q
        )
        scores_doc = jnp.where(mask_doc, scores_doc, MASKED)
        scores_self = jnp.where(mask_self, scores_self, MASKED)
        block_top = jnp.maximum(jnp.max(scores_doc, axis=-1), jnp.max(scores_self, axis=-1))
        weights_doc = jnp.where(mask_doc, jnp.exp(scores_doc - block_top[..., None]), 0.0).astype(
            jnp.bfloat16
        )
        weights_self = jnp.where(
            mask_self, jnp.exp(scores_self - block_top[..., None]), 0.0
        ).astype(jnp.bfloat16)
        block_den = jnp.sum(weights_doc.astype(jnp.float32), axis=-1) + jnp.sum(
            weights_self.astype(jnp.float32), axis=-1
        )
        block_num = jnp.einsum(
            "rgjk,kgd->rgjd", weights_doc, value_doc, preferred_element_type=jnp.float32
        )
        block_num = block_num + jnp.einsum(
            "rgjk,kgd->rgjd", weights_self, value_self, preferred_element_type=jnp.float32
        )
        return (
            block_num.reshape(block_rows, H * HD),
            block_top.reshape(block_rows, H),
            block_den.reshape(block_rows, H),
        )

    starts = jnp.arange(block_count, dtype=jnp.int32) * block_rows
    numer, row_top, denom = lax.map(one_block, starts)
    numer = numer.reshape(total_rows, H * HD)
    row_top = row_top.reshape(total_rows, H)
    denom = denom.reshape(total_rows, H)
    got_num, got_top, got_den = (
        lax.all_to_all(numer[None], "seq", split_axis=1, concat_axis=0, tiled=True),
        lax.all_to_all(row_top[None], "seq", split_axis=1, concat_axis=0, tiled=True),
        lax.all_to_all(denom[None], "seq", split_axis=1, concat_axis=0, tiled=True),
    )
    overall = jnp.max(got_top, axis=0)
    rescale = jnp.exp(got_top - overall[None])
    total_num = jnp.sum(
        got_num.reshape(device_count, rows_local, H, HD) * rescale[:, :, :, None], axis=0
    )
    total_den = jnp.sum(got_den * rescale, axis=0)
    question, position, live_rows, row_offset = row_tables(
        device_index * rows_local, rows_local, lengths, offsets
    )
    safe_den = jnp.where(live_rows[:, None], total_den, 1.0)
    result = (total_num / safe_den[:, :, None]).reshape(rows_local, H * HD)
    return jnp.where(live_rows[:, None], result, 0.0).astype(jnp.bfloat16)


MESH = pl.DeviceIdType.MESH
LANE = 128
CHUNKS = ((0, 2), (2, 2), (4, 2), (6, 2))
GROUPS = 2
PIECES = ((0, 2), (2, 8))
WHOLE = (0, 8)
LOG2E = math.log2(math.e)
WIRE = jnp.int16
WIRE_TOP = 32767.0
HALF_KVH = KVH // 2
PER_GROUP = H // KVH
STATS = 8
QK_TILE = 256


def fused_kernel(
    n, q_hbm, qk_hbm, qv_hbm, k_hbm, v_hbm, len_ref, off_ref, o_ref,
    qown, qbuf, selfs, kv, vt, key_mask, row_mask, scores,
    nkeep, skeep, nsend, narr, wsend, warr, osend, okeep,
    local_sem, kv_sem, kv_recv, once_send, once_recv, zq_recv, f_recv, r_recv, far, p_recv, w_recv,
):
    length = n // 4
    rows = q_hbm.shape[0]
    doc = k_hbm.shape[0]
    docs = 2 * doc
    selves = 2 * rows
    half_kv = HALF_KVH * HD
    half_q = half_kv * PER_GROUP
    unit = PER_GROUP * HD
    side = length * 2 * rows
    me = lax.axis_index("seq")
    core = lax.rem(me, 2)
    chip = me // 2
    y = lax.rem(chip, 2)
    z = chip // 2
    others = (z + 1 - 2 * lax.rem(z, 2), 2 - z // 2, 3 - 3 * (z // 2))

    def device(zz, yy, cc):
        return {"seq": (zz * 2 + yy) * 2 + cc}

    middle = (lax.rem(z, length - 1) + 1) // 2
    across = 1 + lax.rem(z, 2)
    near = others[0]
    kv_sent, self_sent, q_sent, pq_sent, f_sent, r_sent, p_sent, w_sent, o_sent = range(9)
    self_got, yq_got, pq_got, o_got = range(4)

    def await_bytes(ref, sem):
        pltpu.make_async_copy(ref, ref, sem).wait()

    barrier = pltpu.get_barrier_semaphore()
    peers = [device(z, y, 1 - core)] + [device(z, 1 - y, cc) for cc in range(2)]
    peers += [device(near, y, cc) for cc in range(2)]
    for peer in peers:
        pl.semaphore_signal(barrier, inc=1, device_id=peer, device_id_type=MESH)

    @pl.when(middle == 1)
    def greet():
        for cc in range(2):
            pl.semaphore_signal(barrier, inc=1, device_id=device(across, y, cc), device_id_type=MESH)

    q_in = pltpu.make_async_copy(q_hbm, qown, local_sem.at[0])
    q_in.start()
    for i, a in enumerate((qk_hbm, qv_hbm)):
        pltpu.make_async_copy(
            a.at[:, pl.ds(core * half_kv, half_kv)], selfs.at[i, core], local_sem.at[2]
        ).start()

    def part(piece):
        return pl.ds(piece[0] * unit, (piece[1] - piece[0]) * unit)

    def o_local(c):
        cols = pl.ds(CHUNKS[c][0] * unit, CHUNKS[c][1] * unit)
        to = pl.ds(core * half_q + CHUNKS[c][0] * unit, CHUNKS[c][1] * unit)
        return pltpu.make_async_copy(okeep.at[:, cols], o_ref.at[:, to], local_sem.at[3])

    q_own = pltpu.make_async_copy(q_hbm.at[:, pl.ds(core * half_q, half_q)], qbuf.at[y, z, core], local_sem.at[1])

    def kv_cols(side_core, c):
        return pl.ds(side_core * half_kv + CHUNKS[c][0] * HD, CHUNKS[c][1] * HD)

    def kv_part(side_core, c):
        return kv.at[:, pl.ds(side_core * doc, doc), kv_cols(0, c)]

    def kv_local(c):
        at = pl.ds(core * doc, doc)
        return [
            pltpu.make_async_copy(a.at[:, kv_cols(core, c)], kv.at[i, at, kv_cols(0, c)], kv_sem.at[c])
            for i, a in enumerate((k_hbm, v_hbm))
        ]

    def kv_remote(c):
        at = pl.ds(core * doc, doc)
        return [
            pltpu.make_async_remote_copy(
                a.at[:, kv_cols(1 - core, c)], kv.at[i, at, kv_cols(0, c)],
                once_send.at[kv_sent], kv_recv.at[c],
                device_id=device(z, y, 1 - core), device_id_type=MESH,
            )
            for i, a in enumerate((k_hbm, v_hbm))
        ]

    def self_remote():
        cols = pl.ds((1 - core) * half_kv, half_kv)
        return [
            pltpu.make_async_remote_copy(
                a.at[:, cols], selfs.at[i, core], once_send.at[self_sent], once_recv.at[self_got],
                device_id=device(z, y, 1 - core), device_id_type=MESH,
            )
            for i, a in enumerate((qk_hbm, qv_hbm))
        ]

    def q_copy(where, piece, send_sem, recv_sem):
        zz, yy, cc = where
        return pltpu.make_async_remote_copy(
            qown.at[:, pl.ds(cc * half_q + piece[0] * unit, (piece[1] - piece[0]) * unit)],
            qbuf.at[y, z, core, :, part(piece)], send_sem, recv_sem,
            device_id=device(zz, yy, cc), device_id_type=MESH,
        )

    def zq(order, i, piece, cc):
        to = 0 if order == 0 else 2 - middle
        return q_copy((others[order], y, cc), piece, once_send.at[q_sent], zq_recv.at[i, to])

    def yq(cc):
        return q_copy((z, 1 - y, cc), WHOLE, once_send.at[q_sent], once_recv.at[yq_got])

    def pq():
        return q_copy((z, y, 1 - core), WHOLE, once_send.at[pq_sent], once_recv.at[pq_got])

    def forward(order, i, piece):
        zz = others[order]
        return pltpu.make_async_remote_copy(
            qbuf.at[y, zz, :, :, part(piece)], qbuf.at[y, zz, :, :, part(piece)],
            once_send.at[f_sent], f_recv.at[i, order],
            device_id=device(z, 1 - y, core), device_id_type=MESH,
        )

    def along(order, i, piece):
        zz = others[order]
        return pltpu.make_async_remote_copy(
            qbuf.at[y, zz, :, :, part(piece)], qbuf.at[y, zz, :, :, part(piece)],
            once_send.at[r_sent], r_recv.at[i, order - 1],
            device_id=device(near, y, core), device_id_type=MESH,
        )

    def p_copy(c):
        return pltpu.make_async_remote_copy(
            nsend.at[c, pl.ds(0, CHUNKS[c][1] * HD + 16)], narr.at[c, pl.ds(0, CHUNKS[c][1] * HD + 16)],
            once_send.at[p_sent], p_recv.at[c],
            device_id=device(z, 1 - y, core), device_id_type=MESH,
        )

    def w_copy(c, zz):
        return pltpu.make_async_remote_copy(
            wsend.at[c, zz, :, pl.ds(0, CHUNKS[c][1] * unit + LANE)],
            warr.at[c, z, :, pl.ds(0, CHUNKS[c][1] * unit + LANE)], once_send.at[w_sent], w_recv.at[c],
            device_id=device(zz, y, core), device_id_type=MESH,
        )

    def o_copy(c):
        return pltpu.make_async_remote_copy(
            osend.at[:, pl.ds(CHUNKS[c][0] * unit, CHUNKS[c][1] * unit)],
            o_ref.at[:, pl.ds(core * half_q + CHUNKS[c][0] * unit, CHUNKS[c][1] * unit)],
            once_send.at[o_sent], once_recv.at[o_got],
            device_id=device(z, y, 1 - core), device_id_type=MESH,
        )

    q_own.start()
    for c in range(len(CHUNKS)):
        for copy in reversed(kv_local(c)):
            copy.start()
    with jax.named_scope("enter"):
        q_in.wait()
        pl.semaphore_wait(barrier, len(peers) + 2 * middle)

    @pl.when(middle == 1)
    def spread():
        for cc in range(2):
            pl.semaphore_signal(far, inc=1, device_id=device(near, y, cc), device_id_type=MESH)

    for cc in range(2):
        yq(cc).start()
    def send(order, i):
        for cc in range(2):
            zq(order, i, PIECES[i], cc).start()

    early = z < length // 2
    rest = range(1, len(PIECES))
    send(0, 0)

    @pl.when(early)
    def near_rest():
        for i in rest:
            send(0, i)

    pq().start()
    for copy in self_remote():
        copy.start()
    for c in range(len(CHUNKS)):
        for copy in reversed(kv_remote(c)):
            copy.start()

    @pl.when(middle == 0)
    def await_second():
        pl.semaphore_wait(far, 2)

    send(1, 0)

    @pl.when(z >= length // 2)
    def late_rest():
        for i in rest:
            send(0, i)

    for i in rest:
        send(1, i)

    await_bytes(selfs.at[0], local_sem.at[2])
    place = lax.broadcasted_iota(jnp.int32, (docs, LANE), 0)
    lane = lax.broadcasted_iota(jnp.int32, (docs, LANE), 1)
    hidden = (chip * docs + place >= off_ref[0]) & (lane == 0)
    key_mask[:docs, :] = jnp.where(hidden, MASKED, 0.0).astype(key_mask.dtype)
    own = lane[:selves] == place[:selves] + 1
    key_mask[docs:, :] = jnp.where(own, 1.0, 0.0).astype(key_mask.dtype)
    spot, lane = place[: 2 * LANE], lane[: 2 * LANE]
    inner = spot % side
    row = ((inner // (2 * rows)) * 2 + jnp.where(spot < LANE, y, 1 - y)) * (2 * rows) + inner % (2 * rows)
    later = (lane <= selves) & (chip * selves + lane - 1 > row)
    row_mask[...] = jnp.where(lane == 0, 1.0, jnp.where(later, MASKED, 0.0)).astype(row_mask.dtype)
    ones = lax.broadcasted_iota(jnp.int32, (16, docs + LANE), 0) == 0
    ones = jnp.where(ones, 1.0, 0.0).astype(vt.dtype)
    for g in range(HALF_KVH):
        vt[g, HD:, :] = ones
    await_bytes(selfs.at[0], once_recv.at[self_got])
    for i in range(2):
        kv[i, docs:, :] = selfs[i].astype(jnp.float32).reshape(selves, half_kv).astype(kv.dtype)

    def turn(c):
        with jax.named_scope("kv"):
            await_bytes(kv_part(core, c), kv_sem.at[c])
            await_bytes(kv_part(1 - core, c), kv_recv.at[c])
        for g in range(CHUNKS[c][0], sum(CHUNKS[c])):
            cols = slice(g * HD, (g + 1) * HD)
            vt[g, :HD, :docs] = kv[1, :docs, cols].T
            last = kv[1, docs:, cols].astype(jnp.float32)
            last = jnp.concatenate([last, jnp.zeros((LANE - selves, HD), jnp.float32)], axis=0)
            vt[g, :HD, docs:] = last.T.astype(vt.dtype)

    def take(order, i):
        zz = others[order]

        block = qbuf.at[y, zz, :, :, part(PIECES[i])]
        if order == 0:
            await_bytes(block, zq_recv.at[i, 0])
        else:

            @pl.when(middle == 1)
            def hand_on():
                await_bytes(block, zq_recv.at[i, order])
                along(order, i, PIECES[i]).start()

            @pl.when(middle == 0)
            def handed():
                await_bytes(block, r_recv.at[i, order - 1])

        forward(order, i, PIECES[i]).start()

    def relay(c):
        take(0, c)
        if c == 0:

            @pl.when(early)
            def near_too():
                take(0, 1)

        else:
            return
        take(1, 0)
        take(2, 0)

    def relay_rest():
        @pl.when(z >= length // 2)
        def near_now():
            take(0, 1)

        take(1, 1)
        take(2, 1)

    factor = QSCALE ** (-0.5) * LOG2E
    base = me // n
    tile = 256

    def attend(c):
        first, count = CHUNKS[c]
        with jax.named_scope("queries"):
            if c == 0:
                q_own.wait()
                await_bytes(qbuf.at[y, z, 1 - core], once_recv.at[pq_got])
                await_bytes(qbuf.at[1 - y, z], once_recv.at[yq_got])
            for i, piece in enumerate(PIECES):
                if piece[0] == CHUNKS[c][0]:
                    for order in range(3):
                        await_bytes(
                            qbuf.at[1 - y, others[order], :, :, part(piece)], f_recv.at[i, order]
                        )

        def load(g):
            pieces = []
            for yy in (y, 1 - y):
                for j in range(PER_GROUP):
                    h = (first + g) * PER_GROUP + j
                    block = qbuf[yy, :, :, :, h * HD : (h + 1) * HD].astype(jnp.float32)
                    pieces.append(block.reshape(side, HD).astype(jnp.bfloat16))
            return jnp.concatenate([jnp.concatenate(pieces, axis=0), row_mask[...]], axis=1)

        starts = list(range(0, docs, tile)) + [docs]
        q_starts = list(range(0, docs, QK_TILE)) + [docs]

        def score(g, query, start, top):
            at = first + g
            size = QK_TILE if start < docs else selves
            span = slice(start, start + size)
            key = jnp.concatenate([kv[0, span, at * HD : (at + 1) * HD], key_mask[span, :]], axis=1)
            part = lax.dot_general(
                key, query, (((1,), (1,)), ((), ())), preferred_element_type=jnp.float32
            )
            scores[base, at % 2, start : start + size, :] = part
            most = jnp.max(part.reshape(size // 8, 8, 2 * LANE), axis=0)
            return most if top is None else jnp.maximum(top, most)

        def weigh(g, start, top, total):
            at = first + g
            size = span = tile if start < docs else selves
            weights = jnp.exp2((scores[base, at % 2, start : start + size, :] - top) * factor)
            if start == docs:
                span = LANE
                weights = jnp.concatenate(
                    [weights, jnp.zeros((LANE - selves, 2 * LANE), jnp.float32)], axis=0
                )
            got = jnp.dot(
                vt[at, :, start : start + span], weights.astype(jnp.bfloat16),
                preferred_element_type=jnp.float32,
            )
            return got if total is None else total + got

        def begin(g):
            query, after = load(g), None
            for start in q_starts:
                after = score(g, query, start, after)
            return after

        after = begin(0)
        for g in range(count):
            top, total = jnp.max(after, axis=0, keepdims=True), None
            if g + 1 < count:
                after = begin(g + 1)
            for start in starts:
                total = weigh(g, start, top, total)
            top = top * factor
            den = total[HD : HD + 1]
            num = total[:HD]
            nkeep[c, g * HD : (g + 1) * HD, :] = num[:, :LANE]
            skeep[c, 2 * g : 2 * g + 1, :] = top[:, :LANE]
            skeep[c, 2 * g + 1 : 2 * g + 2, :] = den[:, :LANE]
            out = num[:, LANE:]
            largest = jnp.maximum(jnp.max(jnp.abs(out), axis=0, keepdims=True), 1e-30)
            nsend[c, g * HD : (g + 1) * HD, :] = encode(out * (WIRE_TOP / largest))
            skeep[c, 4 + g : 5 + g, :] = top[:, LANE:] + log2(den[:, LANE:])
            skeep[c, 6 + g : 7 + g, :] = top[:, LANE:] + log2(largest)
        logs = split(skeep[c, 4:8, :])
        logs = jnp.concatenate([logs, jnp.zeros((8, LANE), jnp.float32)], axis=0)
        nsend[c, count * HD : count * HD + 16, :] = encode(logs)
        p_copy(c).start()

    def pair_up(c):
        count = CHUNKS[c][1]
        wide = count * unit
        with jax.named_scope("pair"):
            await_bytes(narr.at[c], p_recv.at[c])
        logs = decode(narr[c, count * HD : count * HD + 16, :])
        logs = logs[:4] * COARSE + logs[4:8] * FINE
        mass, span = [], []
        for g in range(count):
            top_a, den_a = skeep[c, 2 * g : 2 * g + 1, :], skeep[c, 2 * g + 1 : 2 * g + 2, :]
            mass_b, span_b = logs[g : g + 1], logs[2 + g : 3 + g]
            top = jnp.maximum(top_a, mass_b)
            fa = jnp.exp2(top_a - top)
            den = den_a * fa + jnp.exp2(mass_b - top)
            fb = jnp.exp2(span_b - top) * (1.0 / WIRE_TOP)
            at = slice(g * HD, (g + 1) * HD)
            num = nkeep[c, at, :] * fa + decode(narr[c, at, :]) * fb
            largest = jnp.maximum(jnp.max(jnp.abs(num), axis=0, keepdims=True), 1e-30)
            codes = encode((num * (WIRE_TOP / largest)).T)
            for j in range(PER_GROUP):
                h = g * PER_GROUP + j
                wsend[c, :, :, h * HD : (h + 1) * HD] = codes[j * side : (j + 1) * side].reshape(
                    length, 2 * rows, HD
                )
            mass.append(top + log2(den))
            span.append(top + log2(largest))
        spare = [jnp.zeros((1, LANE), jnp.float32)] * (GROUPS - count)
        table = split(jnp.concatenate(mass + spare + span + spare, axis=0))
        table = jnp.concatenate([table, jnp.zeros((LANE - 8, LANE), jnp.float32)], axis=0)
        table = encode(table.T)
        for j in range(PER_GROUP):
            wsend[c, :, :, wide + 8 * j : wide + 8 * j + 8] = table[j * side : (j + 1) * side, :8].reshape(
                length, 2 * rows, 8
            )
        for zz in reversed(others):
            w_copy(c, zz).start()
        warr[c, z] = wsend[c, z]

    def finish(c):
        first, count = CHUNKS[c]
        wide = count * unit
        with jax.named_scope("parts"):
            await_bytes(warr.at[c, pl.ds(0, length - 1)], w_recv.at[c])
        logs = []
        for k in range(length):
            block = decode(warr[c, k, :, wide : wide + LANE])
            logs.append(block * COARSE + pltpu.roll(block, LANE - 4, 1) * FINE)
        most = functools.reduce(jnp.maximum, logs)
        den = sum(jnp.exp2(x - most) for x in logs)
        most, den = pltpu.roll(most, 2, 1), pltpu.roll(den, 2, 1)
        share = 1.0 / (den * WIRE_TOP)
        coefs = [jnp.exp2(x - most) * share for x in logs]
        mine = chip * selves + lax.broadcasted_iota(jnp.int32, (selves, HD), 0)
        live = mine < len_ref[0]
        for g in range(count):
            for j in range(PER_GROUP):
                h = g * PER_GROUP + j
                at = 8 * j + 2 + g
                acc = None
                for k in range(length):
                    term = decode(warr[c, k, :, h * HD : (h + 1) * HD]) * coefs[k][:, at : at + 1]
                    acc = term if acc is None else acc + term
                acc = jnp.where(live, acc, 0.0)
                kept = jnp.where(core == 0, acc[:rows], acc[rows:])
                sent = jnp.where(core == 0, acc[rows:], acc[:rows])
                to = first * unit + h * HD
                okeep[:, to : to + HD] = kept.astype(o_ref.dtype)
                osend[:, first * unit + h * HD : first * unit + (h + 1) * HD] = sent.astype(o_ref.dtype)
        o_copy(c).start()
        o_local(c).start()

    def drain():
        await_bytes(kv.at[:, pl.ds(0, doc), :], once_send.at[kv_sent])
        await_bytes(selfs.at[0], once_send.at[self_sent])
        await_bytes(qown.at[:, pl.ds(0, half_q)], once_send.at[pq_sent])
        await_bytes(qbuf.at[0, pl.ds(0, 3)], once_send.at[q_sent])
        await_bytes(qbuf.at[0, pl.ds(0, 3)], once_send.at[f_sent])

        @pl.when(middle == 1)
        def handed_on():
            await_bytes(qbuf.at[0, pl.ds(0, 2)], once_send.at[r_sent])

        await_bytes(nsend, once_send.at[p_sent])

    def run(name, step, c):
        with jax.named_scope(f"{name}#c={c}"):
            step(c)

    run("turn", turn, 0)
    run("relay", relay, 0)
    for c in range(1, len(CHUNKS) - 1):
        run("turn", turn, c)
    with jax.named_scope("relay_rest"):
        relay_rest()
    run("turn", turn, len(CHUNKS) - 1)
    for c in range(len(CHUNKS)):
        run("attend", attend, c)
        if c > 1:
            run("pair_up", pair_up, c - 2)
    for c in range(len(CHUNKS) - 2, len(CHUNKS)):
        run("pair_up", pair_up, c)
    with jax.named_scope("drain"):
        drain()
    for c in range(len(CHUNKS)):
        run("finish", finish, c)
    with jax.named_scope("last"):
        await_bytes(wsend.at[:, pl.ds(0, length - 1)], once_send.at[w_sent])
        await_bytes(osend, once_send.at[o_sent])
        await_bytes(okeep, local_sem.at[3])
        await_bytes(osend, once_recv.at[o_got])


COARSE = 2.0 ** -5
FINE = 2.0 ** -20


def split(x):
    x = jnp.maximum(x, -1000.0)
    high = jnp.round(x * (1.0 / COARSE))
    return jnp.concatenate([high, (x - high * COARSE) * (1.0 / FINE)], axis=0)


def log2(x):
    return jnp.log(x) * LOG2E


def encode(x):
    return jnp.round(x).astype(jnp.int32).astype(WIRE)


def decode(x):
    return x.astype(jnp.int32).astype(jnp.float32)


def fused(n, queries, question_keys, question_values, doc_keys, doc_values, lengths, offsets):
    rows = queries.shape[0]
    doc = doc_keys.shape[0]
    if (
        NQ != 1 or n != 16 or rows % 8 or n * rows * PER_GROUP != 2 * LANE
        or doc % LANE or doc > 1024 or n * rows != QL
    ):
        return local(
            queries, question_keys, question_values, doc_keys, doc_values, lengths, offsets
        )
    operands = (queries, question_keys, question_values, doc_keys, doc_values)
    length = n // 4
    docs, selves = 2 * doc, 2 * rows
    half_kv = HALF_KVH * HD
    wide = GROUPS * PER_GROUP * HD
    hbm = pl.BlockSpec(memory_space=pltpu.HBM)
    smem = pl.BlockSpec(memory_space=pltpu.SMEM)
    f32, bf16 = jnp.float32, jnp.bfloat16
    pieces, chunks = len(PIECES), len(CHUNKS)
    dma = pltpu.SemaphoreType.DMA
    return pl.pallas_call(
        functools.partial(fused_kernel, n),
        out_shape=jax.ShapeDtypeStruct(queries.shape, bf16),
        in_specs=[hbm] * 5 + [smem] * 2,
        out_specs=pl.BlockSpec(memory_space=pl.ANY),
        scratch_shapes=[
            pltpu.VMEM((rows, H * HD), bf16),
            pltpu.VMEM((2, length, 2, rows, half_kv * PER_GROUP), bf16),
            pltpu.VMEM((2, 2, rows, half_kv), bf16),
            pltpu.VMEM((2, docs + selves, half_kv), bf16),
            pltpu.VMEM((HALF_KVH, HD + 16, docs + LANE), bf16),
            pltpu.VMEM((docs + selves, LANE), bf16),
            pltpu.VMEM((2 * LANE, LANE), bf16),
            pltpu.VMEM((1, 2, docs + selves, 2 * LANE), f32),
            pltpu.VMEM((chunks, GROUPS * HD, LANE), f32),
            pltpu.VMEM((chunks, STATS, LANE), f32),
            pltpu.VMEM((chunks, GROUPS * HD + 16, LANE), WIRE),
            pltpu.VMEM((chunks, GROUPS * HD + 16, LANE), WIRE),
            pltpu.VMEM((chunks, length, 2 * rows, wide + LANE), WIRE),
            pltpu.VMEM((chunks, length, 2 * rows, wide + LANE), WIRE),
            pltpu.VMEM((rows, half_kv * PER_GROUP), bf16),
            pltpu.VMEM((rows, half_kv * PER_GROUP), bf16),
            dma((4,)),
            dma((chunks,)),
            dma((chunks,)),
            dma((9,)),
            dma((4,)),
            dma((pieces, 3)),
            dma((pieces, 3)),
            dma((pieces, 2)),
            pltpu.SemaphoreType.REGULAR,
            dma((chunks,)),
            dma((chunks,)),
        ],
        compiler_params=pltpu.CompilerParams(
            collective_id=0, has_side_effects=True, vmem_limit_bytes=24 * 1024 * 1024
        ),
    )(*(pltpu.with_memory_space_constraint(x, pltpu.HBM) for x in operands), lengths, offsets)


def solution(mesh):
    placed = (
        P(("grp", "seq"), None),
        P(("grp", "seq"), None),
        P(("grp", "seq"), None),
        P(("grp", "seq"), None),
        P(("grp", "seq"), None),
        P("grp"),
        P("grp"),
    )
    return jax.shard_map(
        functools.partial(fused, mesh.shape["seq"]),
        mesh=mesh, in_specs=placed, out_specs=P(("grp", "seq"), None), check_vma=False,
    )
```

```python
import functools
import math

import jax
import jax.numpy as jnp
from jax import lax
from jax.experimental import pallas as pl
from jax.experimental.pallas import tpu as pltpu
from jax.sharding import PartitionSpec as P

H = 32
KVH = 16
HD = 128
QSCALE = 144
QL = 128
NQ = 1


MASKED = -1e30


def row_tables(start, count, lengths, offsets):
    rows = start + jnp.arange(count, dtype=jnp.int32)
    question = rows // QL
    position = rows % QL
    owner_table = question[:, None] == jnp.arange(NQ, dtype=jnp.int32)[None, :]
    row_length = jnp.sum(jnp.where(owner_table, lengths[None, :], 0), axis=1)
    row_offset = jnp.sum(jnp.where(owner_table, offsets[None, :], 0), axis=1)
    return (question, position, position < row_length, row_offset)


def local(queries, question_keys, question_values, doc_keys, doc_values, lengths, offsets):
    rows_local = queries.shape[0]
    doc_local = doc_keys.shape[0]
    device_count = lax.axis_size("seq")
    device_index = lax.axis_index("seq")
    total_rows = rows_local * device_count
    per_group = H // KVH
    factor_q = QSCALE ** (-0.5)
    key_doc = doc_keys.reshape(doc_local, KVH, HD)
    value_doc = doc_values.reshape(doc_local, KVH, HD)
    key_self = question_keys.reshape(rows_local, KVH, HD)
    value_self = question_values.reshape(rows_local, KVH, HD)
    doc_places = device_index * doc_local + jnp.arange(doc_local, dtype=jnp.int32)
    self_rows = device_index * rows_local + jnp.arange(rows_local, dtype=jnp.int32)
    whole = lax.all_gather(queries, "seq", axis=0, tiled=True)
    block_rows = math.gcd(total_rows, 512)
    block_count = total_rows // block_rows

    def one_block(start):
        piece = whole.reshape(block_rows, KVH, per_group, HD)
        question, position, live_rows, row_offset = row_tables(start, block_rows, lengths, offsets)
        mask_doc = live_rows[:, None] & (doc_places[None, :] < row_offset[:, None])
        mask_self = (
            live_rows[:, None]
            & (self_rows[None, :] // QL == question[:, None])
            & (self_rows[None, :] % QL <= position[:, None])
        )
        mask_doc = mask_doc[:, None, None, :]
        mask_self = mask_self[:, None, None, :]
        scores_doc = (
            jnp.einsum("rgjd,kgd->rgjk", piece, key_doc, preferred_element_type=jnp.float32)
            * factor_q
        )
        scores_self = (
            jnp.einsum("rgjd,kgd->rgjk", piece, key_self, preferred_element_type=jnp.float32)
            * factor_q
        )
        scores_doc = jnp.where(mask_doc, scores_doc, MASKED)
        scores_self = jnp.where(mask_self, scores_self, MASKED)
        block_top = jnp.maximum(jnp.max(scores_doc, axis=-1), jnp.max(scores_self, axis=-1))
        weights_doc = jnp.where(mask_doc, jnp.exp(scores_doc - block_top[..., None]), 0.0).astype(
            jnp.bfloat16
        )
        weights_self = jnp.where(
            mask_self, jnp.exp(scores_self - block_top[..., None]), 0.0
        ).astype(jnp.bfloat16)
        block_den = jnp.sum(weights_doc.astype(jnp.float32), axis=-1) + jnp.sum(
            weights_self.astype(jnp.float32), axis=-1
        )
        block_num = jnp.einsum(
            "rgjk,kgd->rgjd", weights_doc, value_doc, preferred_element_type=jnp.float32
        )
        block_num = block_num + jnp.einsum(
            "rgjk,kgd->rgjd", weights_self, value_self, preferred_element_type=jnp.float32
        )
        return (
            block_num.reshape(block_rows, H * HD),
            block_top.reshape(block_rows, H),
            block_den.reshape(block_rows, H),
        )

    starts = jnp.arange(block_count, dtype=jnp.int32) * block_rows
    numer, row_top, denom = lax.map(one_block, starts)
    numer = numer.reshape(total_rows, H * HD)
    row_top = row_top.reshape(total_rows, H)
    denom = denom.reshape(total_rows, H)
    got_num, got_top, got_den = (
        lax.all_to_all(numer[None], "seq", split_axis=1, concat_axis=0, tiled=True),
        lax.all_to_all(row_top[None], "seq", split_axis=1, concat_axis=0, tiled=True),
        lax.all_to_all(denom[None], "seq", split_axis=1, concat_axis=0, tiled=True),
    )
    overall = jnp.max(got_top, axis=0)
    rescale = jnp.exp(got_top - overall[None])
    total_num = jnp.sum(
        got_num.reshape(device_count, rows_local, H, HD) * rescale[:, :, :, None], axis=0
    )
    total_den = jnp.sum(got_den * rescale, axis=0)
    question, position, live_rows, row_offset = row_tables(
        device_index * rows_local, rows_local, lengths, offsets
    )
    safe_den = jnp.where(live_rows[:, None], total_den, 1.0)
    result = (total_num / safe_den[:, :, None]).reshape(rows_local, H * HD)
    return jnp.where(live_rows[:, None], result, 0.0).astype(jnp.bfloat16)


MESH = pl.DeviceIdType.MESH
LANE = 128
CHUNKS = ((0, 2), (2, 2), (4, 2), (6, 2))
GROUPS = 2
PIECES = ((0, 2), (2, 4), (4, 8))
WHOLE = (0, 8)
LOG2E = math.log2(math.e)
WIRE = jnp.int16
WIRE_TOP = 32767.0
HALF_KVH = KVH // 2
PER_GROUP = H // KVH
STATS = 8
QK_TILE = 256


def fused_kernel(
    n, q_hbm, qk_hbm, qv_hbm, k_hbm, v_hbm, len_ref, off_ref, o_ref,
    qown, qbuf, selfs, kv, vt, key_mask, row_mask, scores,
    nkeep, skeep, nsend, narr, wsend, warr, osend, okeep,
    local_sem, kv_sem, kv_recv, once_send, once_recv, zq_recv, f_recv, r_recv, far, p_recv, w_recv,
):
    length = n // 4
    rows = q_hbm.shape[0]
    doc = k_hbm.shape[0]
    docs = 2 * doc
    selves = 2 * rows
    half_kv = HALF_KVH * HD
    half_q = half_kv * PER_GROUP
    unit = PER_GROUP * HD
    side = length * 2 * rows
    me = lax.axis_index("seq")
    core = lax.rem(me, 2)
    chip = me // 2
    y = lax.rem(chip, 2)
    z = chip // 2
    others = (z + 1 - 2 * lax.rem(z, 2), 2 - z // 2, 3 - 3 * (z // 2))

    def device(zz, yy, cc):
        return {"seq": (zz * 2 + yy) * 2 + cc}

    middle = (lax.rem(z, length - 1) + 1) // 2
    across = 1 + lax.rem(z, 2)
    near = others[0]
    kv_sent, self_sent, q_sent, pq_sent, f_sent, r_sent, p_sent, w_sent, o_sent = range(9)
    self_got, yq_got, pq_got, o_got = range(4)

    def await_bytes(ref, sem):
        pltpu.make_async_copy(ref, ref, sem).wait()

    barrier = pltpu.get_barrier_semaphore()
    peers = [device(z, y, 1 - core)] + [device(z, 1 - y, cc) for cc in range(2)]
    peers += [device(near, y, cc) for cc in range(2)]
    for peer in peers:
        pl.semaphore_signal(barrier, inc=1, device_id=peer, device_id_type=MESH)

    @pl.when(middle == 1)
    def greet():
        for cc in range(2):
            pl.semaphore_signal(barrier, inc=1, device_id=device(across, y, cc), device_id_type=MESH)

    q_in = pltpu.make_async_copy(q_hbm, qown, local_sem.at[0])
    q_in.start()
    for i, a in enumerate((qk_hbm, qv_hbm)):
        pltpu.make_async_copy(
            a.at[:, pl.ds(core * half_kv, half_kv)], selfs.at[i, core], local_sem.at[2]
        ).start()

    def part(piece):
        return pl.ds(piece[0] * unit, (piece[1] - piece[0]) * unit)

    def o_local(c):
        cols = pl.ds(CHUNKS[c][0] * unit, CHUNKS[c][1] * unit)
        to = pl.ds(core * half_q + CHUNKS[c][0] * unit, CHUNKS[c][1] * unit)
        return pltpu.make_async_copy(okeep.at[:, cols], o_ref.at[:, to], local_sem.at[3])

    q_own = pltpu.make_async_copy(q_hbm.at[:, pl.ds(core * half_q, half_q)], qbuf.at[y, z, core], local_sem.at[1])

    def kv_cols(side_core, c):
        return pl.ds(side_core * half_kv + CHUNKS[c][0] * HD, CHUNKS[c][1] * HD)

    def kv_part(side_core, c):
        return kv.at[:, pl.ds(side_core * doc, doc), kv_cols(0, c)]

    def kv_local(c):
        at = pl.ds(core * doc, doc)
        return [
            pltpu.make_async_copy(a.at[:, kv_cols(core, c)], kv.at[i, at, kv_cols(0, c)], kv_sem.at[c])
            for i, a in enumerate((k_hbm, v_hbm))
        ]

    def kv_remote(c):
        at = pl.ds(core * doc, doc)
        return [
            pltpu.make_async_remote_copy(
                a.at[:, kv_cols(1 - core, c)], kv.at[i, at, kv_cols(0, c)],
                once_send.at[kv_sent], kv_recv.at[c],
                device_id=device(z, y, 1 - core), device_id_type=MESH,
            )
            for i, a in enumerate((k_hbm, v_hbm))
        ]

    def self_remote():
        cols = pl.ds((1 - core) * half_kv, half_kv)
        return [
            pltpu.make_async_remote_copy(
                a.at[:, cols], selfs.at[i, core], once_send.at[self_sent], once_recv.at[self_got],
                device_id=device(z, y, 1 - core), device_id_type=MESH,
            )
            for i, a in enumerate((qk_hbm, qv_hbm))
        ]

    def q_copy(where, piece, send_sem, recv_sem):
        zz, yy, cc = where
        return pltpu.make_async_remote_copy(
            qown.at[:, pl.ds(cc * half_q + piece[0] * unit, (piece[1] - piece[0]) * unit)],
            qbuf.at[y, z, core, :, part(piece)], send_sem, recv_sem,
            device_id=device(zz, yy, cc), device_id_type=MESH,
        )

    def zq(order, i, piece, cc):
        to = 0 if order == 0 else 2 - middle
        return q_copy((others[order], y, cc), piece, once_send.at[q_sent], zq_recv.at[i, to])

    def yq(cc):
        return q_copy((z, 1 - y, cc), WHOLE, once_send.at[q_sent], once_recv.at[yq_got])

    def pq():
        return q_copy((z, y, 1 - core), WHOLE, once_send.at[pq_sent], once_recv.at[pq_got])

    def forward(order, i, piece):
        zz = others[order]
        return pltpu.make_async_remote_copy(
            qbuf.at[y, zz, :, :, part(piece)], qbuf.at[y, zz, :, :, part(piece)],
            once_send.at[f_sent], f_recv.at[i, order],
            device_id=device(z, 1 - y, core), device_id_type=MESH,
        )

    def along(order, i, piece):
        zz = others[order]
        return pltpu.make_async_remote_copy(
            qbuf.at[y, zz, :, :, part(piece)], qbuf.at[y, zz, :, :, part(piece)],
            once_send.at[r_sent], r_recv.at[i, order - 1],
            device_id=device(near, y, core), device_id_type=MESH,
        )

    def p_copy(c):
        return pltpu.make_async_remote_copy(
            nsend.at[c, pl.ds(0, CHUNKS[c][1] * HD + 16)], narr.at[c, pl.ds(0, CHUNKS[c][1] * HD + 16)],
            once_send.at[p_sent], p_recv.at[c],
            device_id=device(z, 1 - y, core), device_id_type=MESH,
        )

    def w_copy(c, zz):
        return pltpu.make_async_remote_copy(
            wsend.at[c, zz, :, pl.ds(0, CHUNKS[c][1] * unit + LANE)],
            warr.at[c, z, :, pl.ds(0, CHUNKS[c][1] * unit + LANE)], once_send.at[w_sent], w_recv.at[c],
            device_id=device(zz, y, core), device_id_type=MESH,
        )

    def o_copy(c):
        return pltpu.make_async_remote_copy(
            osend.at[:, pl.ds(CHUNKS[c][0] * unit, CHUNKS[c][1] * unit)],
            o_ref.at[:, pl.ds(core * half_q + CHUNKS[c][0] * unit, CHUNKS[c][1] * unit)],
            once_send.at[o_sent], once_recv.at[o_got],
            device_id=device(z, y, 1 - core), device_id_type=MESH,
        )

    q_own.start()
    for c in range(len(CHUNKS)):
        for copy in reversed(kv_local(c)):
            copy.start()
    with jax.named_scope("enter"):
        q_in.wait()
        pl.semaphore_wait(barrier, len(peers) + 2 * middle)

    @pl.when(middle == 1)
    def spread():
        for cc in range(2):
            pl.semaphore_signal(far, inc=1, device_id=device(near, y, cc), device_id_type=MESH)

    for cc in range(2):
        yq(cc).start()
    def send(order, i):
        for cc in range(2):
            zq(order, i, PIECES[i], cc).start()

    early = z < length // 2
    rest = range(1, len(PIECES))
    send(0, 0)

    @pl.when(early)
    def near_rest():
        for i in rest:
            send(0, i)

    pq().start()
    for copy in self_remote():
        copy.start()
    for c in range(len(CHUNKS)):
        for copy in reversed(kv_remote(c)):
            copy.start()

    @pl.when(middle == 0)
    def await_second():
        pl.semaphore_wait(far, 2)

    send(1, 0)

    for i in rest:
        send(1, i)

    @pl.when(z >= length // 2)
    def late_rest():
        for i in rest:
            send(0, i)

    await_bytes(selfs.at[0], local_sem.at[2])
    place = lax.broadcasted_iota(jnp.int32, (docs, LANE), 0)
    lane = lax.broadcasted_iota(jnp.int32, (docs, LANE), 1)
    hidden = (chip * docs + place >= off_ref[0]) & (lane == 0)
    key_mask[:docs, :] = jnp.where(hidden, MASKED, 0.0).astype(key_mask.dtype)
    own = lane[:selves] == place[:selves] + 1
    key_mask[docs:, :] = jnp.where(own, 1.0, 0.0).astype(key_mask.dtype)
    spot, lane = place[: 2 * LANE], lane[: 2 * LANE]
    inner = spot % side
    row = ((inner // (2 * rows)) * 2 + jnp.where(spot < LANE, y, 1 - y)) * (2 * rows) + inner % (2 * rows)
    later = (lane <= selves) & (chip * selves + lane - 1 > row)
    row_mask[...] = jnp.where(lane == 0, 1.0, jnp.where(later, MASKED, 0.0)).astype(row_mask.dtype)
    ones = lax.broadcasted_iota(jnp.int32, (16, docs + LANE), 0) == 0
    ones = jnp.where(ones, 1.0, 0.0).astype(vt.dtype)
    for g in range(HALF_KVH):
        vt[g, HD:, :] = ones
    await_bytes(selfs.at[0], once_recv.at[self_got])
    for i in range(2):
        kv[i, docs:, :] = selfs[i].astype(jnp.float32).reshape(selves, half_kv).astype(kv.dtype)

    def turn(c):
        with jax.named_scope("kv"):
            await_bytes(kv_part(core, c), kv_sem.at[c])
            await_bytes(kv_part(1 - core, c), kv_recv.at[c])
        for g in range(CHUNKS[c][0], sum(CHUNKS[c])):
            cols = slice(g * HD, (g + 1) * HD)
            vt[g, :HD, :docs] = kv[1, :docs, cols].T
            last = kv[1, docs:, cols].astype(jnp.float32)
            last = jnp.concatenate([last, jnp.zeros((LANE - selves, HD), jnp.float32)], axis=0)
            vt[g, :HD, docs:] = last.T.astype(vt.dtype)

    def take(order, i):
        zz = others[order]

        block = qbuf.at[y, zz, :, :, part(PIECES[i])]
        if order == 0:
            await_bytes(block, zq_recv.at[i, 0])
        else:

            @pl.when(middle == 1)
            def hand_on():
                await_bytes(block, zq_recv.at[i, order])
                along(order, i, PIECES[i]).start()

            @pl.when(middle == 0)
            def handed():
                await_bytes(block, r_recv.at[i, order - 1])

        forward(order, i, PIECES[i]).start()

    def relay():
        take(0, 0)

        @pl.when(early)
        def near_too():
            for i in rest:
                take(0, i)

        take(1, 0)
        take(2, 0)

    def relay_rest():
        late = z >= length // 2

        @pl.when(late & (middle == 0))
        def near_now():
            for i in rest:
                take(0, i)

        for i in rest:
            take(1, i)
            take(2, i)

        @pl.when(late & (middle == 1))
        def near_last():
            for i in rest:
                take(0, i)

    factor = QSCALE ** (-0.5) * LOG2E
    base = me // n
    tile = 256

    def attend(c):
        first, count = CHUNKS[c]
        with jax.named_scope("queries"):
            if c == 0:
                q_own.wait()
                await_bytes(qbuf.at[y, z, 1 - core], once_recv.at[pq_got])
                await_bytes(qbuf.at[1 - y, z], once_recv.at[yq_got])
            for i, piece in enumerate(PIECES):
                if piece[0] == CHUNKS[c][0]:
                    for order in range(3):
                        await_bytes(
                            qbuf.at[1 - y, others[order], :, :, part(piece)], f_recv.at[i, order]
                        )

        def load(g):
            pieces = []
            for yy in (y, 1 - y):
                for j in range(PER_GROUP):
                    h = (first + g) * PER_GROUP + j
                    block = qbuf[yy, :, :, :, h * HD : (h + 1) * HD].astype(jnp.float32)
                    pieces.append(block.reshape(side, HD).astype(jnp.bfloat16))
            return jnp.concatenate([jnp.concatenate(pieces, axis=0), row_mask[...]], axis=1)

        starts = list(range(0, docs, tile)) + [docs]
        q_starts = list(range(0, docs, QK_TILE)) + [docs]

        def score(g, query, start, top):
            at = first + g
            size = QK_TILE if start < docs else selves
            span = slice(start, start + size)
            key = jnp.concatenate([kv[0, span, at * HD : (at + 1) * HD], key_mask[span, :]], axis=1)
            part = lax.dot_general(
                key, query, (((1,), (1,)), ((), ())), preferred_element_type=jnp.float32
            )
            scores[base, at % 2, start : start + size, :] = part
            most = jnp.max(part.reshape(size // 8, 8, 2 * LANE), axis=0)
            return most if top is None else jnp.maximum(top, most)

        def weigh(g, start, top, total):
            at = first + g
            size = span = tile if start < docs else selves
            weights = jnp.exp2((scores[base, at % 2, start : start + size, :] - top) * factor)
            if start == docs:
                span = LANE
                weights = jnp.concatenate(
                    [weights, jnp.zeros((LANE - selves, 2 * LANE), jnp.float32)], axis=0
                )
            got = jnp.dot(
                vt[at, :, start : start + span], weights.astype(jnp.bfloat16),
                preferred_element_type=jnp.float32,
            )
            return got if total is None else total + got

        def begin(g):
            query, after = load(g), None
            for start in q_starts:
                after = score(g, query, start, after)
            return after

        after = begin(0)
        for g in range(count):
            top, total = jnp.max(after, axis=0, keepdims=True), None
            if g + 1 < count:
                after = begin(g + 1)
            for start in starts:
                total = weigh(g, start, top, total)
            top = top * factor
            den = total[HD : HD + 1]
            num = total[:HD]
            nkeep[c, g * HD : (g + 1) * HD, :] = num[:, :LANE]
            skeep[c, 2 * g : 2 * g + 1, :] = top[:, :LANE]
            skeep[c, 2 * g + 1 : 2 * g + 2, :] = den[:, :LANE]
            out = num[:, LANE:]
            largest = jnp.maximum(jnp.max(jnp.abs(out), axis=0, keepdims=True), 1e-30)
            nsend[c, g * HD : (g + 1) * HD, :] = encode(out * (WIRE_TOP / largest))
            skeep[c, 4 + g : 5 + g, :] = top[:, LANE:] + log2(den[:, LANE:])
            skeep[c, 6 + g : 7 + g, :] = top[:, LANE:] + log2(largest)
        logs = split(skeep[c, 4:8, :])
        logs = jnp.concatenate([logs, jnp.zeros((8, LANE), jnp.float32)], axis=0)
        nsend[c, count * HD : count * HD + 16, :] = encode(logs)
        p_copy(c).start()

    def pair_up(c):
        count = CHUNKS[c][1]
        wide = count * unit
        with jax.named_scope("pair"):
            await_bytes(narr.at[c], p_recv.at[c])
        logs = decode(narr[c, count * HD : count * HD + 16, :])
        logs = logs[:4] * COARSE + logs[4:8] * FINE
        mass, span = [], []
        for g in range(count):
            top_a, den_a = skeep[c, 2 * g : 2 * g + 1, :], skeep[c, 2 * g + 1 : 2 * g + 2, :]
            mass_b, span_b = logs[g : g + 1], logs[2 + g : 3 + g]
            top = jnp.maximum(top_a, mass_b)
            fa = jnp.exp2(top_a - top)
            den = den_a * fa + jnp.exp2(mass_b - top)
            fb = jnp.exp2(span_b - top) * (1.0 / WIRE_TOP)
            at = slice(g * HD, (g + 1) * HD)
            num = nkeep[c, at, :] * fa + decode(narr[c, at, :]) * fb
            largest = jnp.maximum(jnp.max(jnp.abs(num), axis=0, keepdims=True), 1e-30)
            codes = encode((num * (WIRE_TOP / largest)).T)
            for j in range(PER_GROUP):
                h = g * PER_GROUP + j
                wsend[c, :, :, h * HD : (h + 1) * HD] = codes[j * side : (j + 1) * side].reshape(
                    length, 2 * rows, HD
                )
            mass.append(top + log2(den))
            span.append(top + log2(largest))
        spare = [jnp.zeros((1, LANE), jnp.float32)] * (GROUPS - count)
        table = split(jnp.concatenate(mass + spare + span + spare, axis=0))
        table = jnp.concatenate([table, jnp.zeros((LANE - 8, LANE), jnp.float32)], axis=0)
        table = encode(table.T)
        for j in range(PER_GROUP):
            wsend[c, :, :, wide + 8 * j : wide + 8 * j + 8] = table[j * side : (j + 1) * side, :8].reshape(
                length, 2 * rows, 8
            )
        for zz in reversed(others):
            w_copy(c, zz).start()
        warr[c, z] = wsend[c, z]

    def finish(c):
        first, count = CHUNKS[c]
        wide = count * unit
        with jax.named_scope("parts"):
            await_bytes(warr.at[c, pl.ds(0, length - 1)], w_recv.at[c])
        logs = []
        for k in range(length):
            block = decode(warr[c, k, :, wide : wide + LANE])
            logs.append(block * COARSE + pltpu.roll(block, LANE - 4, 1) * FINE)
        most = functools.reduce(jnp.maximum, logs)
        den = sum(jnp.exp2(x - most) for x in logs)
        most, den = pltpu.roll(most, 2, 1), pltpu.roll(den, 2, 1)
        share = 1.0 / (den * WIRE_TOP)
        coefs = [jnp.exp2(x - most) * share for x in logs]
        mine = chip * selves + lax.broadcasted_iota(jnp.int32, (selves, HD), 0)
        live = mine < len_ref[0]
        for g in range(count):
            for j in range(PER_GROUP):
                h = g * PER_GROUP + j
                at = 8 * j + 2 + g
                acc = None
                for k in range(length):
                    term = decode(warr[c, k, :, h * HD : (h + 1) * HD]) * coefs[k][:, at : at + 1]
                    acc = term if acc is None else acc + term
                acc = jnp.where(live, acc, 0.0)
                kept = jnp.where(core == 0, acc[:rows], acc[rows:])
                sent = jnp.where(core == 0, acc[rows:], acc[:rows])
                to = first * unit + h * HD
                okeep[:, to : to + HD] = kept.astype(o_ref.dtype)
                osend[:, first * unit + h * HD : first * unit + (h + 1) * HD] = sent.astype(o_ref.dtype)
        o_copy(c).start()
        o_local(c).start()

    def drain():
        await_bytes(kv.at[:, pl.ds(0, doc), :], once_send.at[kv_sent])
        await_bytes(selfs.at[0], once_send.at[self_sent])
        await_bytes(qown.at[:, pl.ds(0, half_q)], once_send.at[pq_sent])
        await_bytes(qbuf.at[0, pl.ds(0, 3)], once_send.at[q_sent])
        await_bytes(qbuf.at[0, pl.ds(0, 3)], once_send.at[f_sent])

        @pl.when(middle == 1)
        def handed_on():
            await_bytes(qbuf.at[0, pl.ds(0, 2)], once_send.at[r_sent])

        await_bytes(nsend, once_send.at[p_sent])

    def run(name, step, c):
        with jax.named_scope(f"{name}#c={c}"):
            step(c)

    run("turn", turn, 0)
    with jax.named_scope("relay"):
        relay()
    for c in range(1, len(CHUNKS) - 1):
        run("turn", turn, c)
    with jax.named_scope("relay_rest"):
        relay_rest()
    run("turn", turn, len(CHUNKS) - 1)
    for c in range(len(CHUNKS)):
        run("attend", attend, c)
    for c in range(len(CHUNKS)):
        run("pair_up", pair_up, c)
    with jax.named_scope("drain"):
        drain()
    for c in range(len(CHUNKS)):
        run("finish", finish, c)
    with jax.named_scope("last"):
        await_bytes(wsend.at[:, pl.ds(0, length - 1)], once_send.at[w_sent])
        await_bytes(osend, once_send.at[o_sent])
        await_bytes(okeep, local_sem.at[3])
        await_bytes(osend, once_recv.at[o_got])


COARSE = 2.0 ** -5
FINE = 2.0 ** -20


def split(x):
    x = jnp.maximum(x, -1000.0)
    high = jnp.round(x * (1.0 / COARSE))
    return jnp.concatenate([high, (x - high * COARSE) * (1.0 / FINE)], axis=0)


def log2(x):
    return jnp.log(x) * LOG2E


def encode(x):
    return jnp.round(x).astype(jnp.int32).astype(WIRE)


def decode(x):
    return x.astype(jnp.int32).astype(jnp.float32)


def fused(n, queries, question_keys, question_values, doc_keys, doc_values, lengths, offsets):
    rows = queries.shape[0]
    doc = doc_keys.shape[0]
    if (
        NQ != 1 or n != 16 or rows % 8 or n * rows * PER_GROUP != 2 * LANE
        or doc % LANE or doc > 1024 or n * rows != QL
    ):
        return local(
            queries, question_keys, question_values, doc_keys, doc_values, lengths, offsets
        )
    operands = (queries, question_keys, question_values, doc_keys, doc_values)
    length = n // 4
    docs, selves = 2 * doc, 2 * rows
    half_kv = HALF_KVH * HD
    wide = GROUPS * PER_GROUP * HD
    hbm = pl.BlockSpec(memory_space=pltpu.HBM)
    smem = pl.BlockSpec(memory_space=pltpu.SMEM)
    f32, bf16 = jnp.float32, jnp.bfloat16
    pieces, chunks = len(PIECES), len(CHUNKS)
    dma = pltpu.SemaphoreType.DMA
    return pl.pallas_call(
        functools.partial(fused_kernel, n),
        out_shape=jax.ShapeDtypeStruct(queries.shape, bf16),
        in_specs=[hbm] * 5 + [smem] * 2,
        out_specs=pl.BlockSpec(memory_space=pl.ANY),
        scratch_shapes=[
            pltpu.VMEM((rows, H * HD), bf16),
            pltpu.VMEM((2, length, 2, rows, half_kv * PER_GROUP), bf16),
            pltpu.VMEM((2, 2, rows, half_kv), bf16),
            pltpu.VMEM((2, docs + selves, half_kv), bf16),
            pltpu.VMEM((HALF_KVH, HD + 16, docs + LANE), bf16),
            pltpu.VMEM((docs + selves, LANE), bf16),
            pltpu.VMEM((2 * LANE, LANE), bf16),
            pltpu.VMEM((1, 2, docs + selves, 2 * LANE), f32),
            pltpu.VMEM((chunks, GROUPS * HD, LANE), f32),
            pltpu.VMEM((chunks, STATS, LANE), f32),
            pltpu.VMEM((chunks, GROUPS * HD + 16, LANE), WIRE),
            pltpu.VMEM((chunks, GROUPS * HD + 16, LANE), WIRE),
            pltpu.VMEM((chunks, length, 2 * rows, wide + LANE), WIRE),
            pltpu.VMEM((chunks, length, 2 * rows, wide + LANE), WIRE),
            pltpu.VMEM((rows, half_kv * PER_GROUP), bf16),
            pltpu.VMEM((rows, half_kv * PER_GROUP), bf16),
            dma((4,)),
            dma((chunks,)),
            dma((chunks,)),
            dma((9,)),
            dma((4,)),
            dma((pieces, 3)),
            dma((pieces, 3)),
            dma((pieces, 2)),
            pltpu.SemaphoreType.REGULAR,
            dma((chunks,)),
            dma((chunks,)),
        ],
        compiler_params=pltpu.CompilerParams(
            collective_id=0, has_side_effects=True, vmem_limit_bytes=24 * 1024 * 1024
        ),
    )(*(pltpu.with_memory_space_constraint(x, pltpu.HBM) for x in operands), lengths, offsets)


def solution(mesh):
    placed = (
        P(("grp", "seq"), None),
        P(("grp", "seq"), None),
        P(("grp", "seq"), None),
        P(("grp", "seq"), None),
        P(("grp", "seq"), None),
        P("grp"),
        P("grp"),
    )
    return jax.shard_map(
        functools.partial(fused, mesh.shape["seq"]),
        mesh=mesh, in_specs=placed, out_specs=P(("grp", "seq"), None), check_vma=False,
    )
```
